32 devices in a mesh: bond: 8 (over z, x), row: 4 (over y, core).
Axes of the slice: x: 2, y: 2, z: 4, core: 2. Of those that a mesh axis runs over, the one named last changes fastest.
Arguments:
- left_site: bfloat16 [16384, 1024], P(('bond', 'row')), may hold values from -6 to 6
- right_site: bfloat16 [8192, 2048], P(('bond', 'row')), may hold values from -0.1875 to 0.1875
- gate: float32 [4, 4], replicated, may hold values from -3 to 3
- omega: bfloat16 [2048, 1024], P(('bond', 'row')), may hold values from -0.125 to 0.125
Outputs:
- left_new: bfloat16 [16384, 1024], P(('bond', 'row'))
- right_new: bfloat16 [8192, 2048], P(('bond', 'row'))
- odd_pair: bfloat16 [16384, 2048], P(('bond', 'row'))
The draws below stay inside these ranges and needn't reach their ends.
All inputs are finite; a program needn't handle non-finite values.
Results may differ from the reference program's by a relative error of at most 0.03.
Values may be sent and summed in bfloat16 or wider, within the bound.
A program may use at most 128 MiB of HBM per device.

```python
import math
import jax
import jax.numpy as jnp
from jax import lax

C = 1024
K = 1024
BONDS = 8


def block_levels(rng, dims, shards, least, largest):
    factor_of = 1.0
    for position, parts in shards:
        heights = jax.random.uniform(jax.random.fold_in(jax.random.fold_in(rng, 6), position), (parts,), jnp.float32, least / len(shards), largest / len(shards))
        factor_of = factor_of * jnp.repeat(jnp.exp(heights), dims[position] // parts).reshape((-1,) + (1,) * (len(dims) - 1 - position))
    return factor_of


def noise(rng, shape, scale, bound, shards=(), kind=jnp.bfloat16):
    values = jax.random.normal(rng, shape, jnp.float32) * scale
    if len(shards) > 0:
        values = block_levels(rng, shape, shards, -0.22, 0.18) * values
    return jnp.clip(values, min=-bound, max=bound).astype(kind)


def setup_inputs(seed: int = 0) -> dict:
    key_list = jax.random.split(jax.random.key(seed), 5)
    return {
        "left_site": noise(key_list[0], (BONDS * 2 * C, C), 1.0, 6.0, ((0, 32),)),
        "right_site": noise(key_list[1], (BONDS * C, 2 * C), C ** -0.5, 0.1875, ((0, 32),)),
        "gate": noise(key_list[2], (4, 4), 0.5, 3.0, (), jnp.float32),
        "omega": noise(key_list[3], (2 * C, K), (2 * C) ** -0.5, 0.125, ((0, 32),)),
    }


def one_bond(pair_in, gate, omega):
    left_one, right_one = pair_in
    product = jnp.dot(left_one.astype(jnp.float32), right_one.astype(jnp.float32), preferred_element_type=jnp.float32)
    mixed = jnp.einsum('stuv,auvc->astc', gate.reshape(2, 2, 2, 2).astype(jnp.float32), product.reshape(C, 2, 2, 2 * C // 2))
    theta = mixed.reshape(2 * C, 2 * C).astype(jnp.bfloat16)
    sketch = jnp.dot(theta.astype(jnp.float32), omega.astype(jnp.float32), preferred_element_type=jnp.float32)
    gram = jnp.dot(sketch.T, sketch, precision=lax.Precision.HIGHEST) / (2.0 * C)
    diag_mean = jnp.trace(gram) / K
    lower = jnp.linalg.cholesky(gram + 0.01 * diag_mean * jnp.eye(K, dtype=gram.dtype))
    basis = lax.linalg.triangular_solve(lower, sketch, left_side=False, lower=True, transpose_a=True)
    left_out = basis.astype(jnp.bfloat16)
    right_out = (jnp.dot(left_out.T.astype(jnp.float32), theta.astype(jnp.float32), preferred_element_type=jnp.float32) * (1.0 / math.sqrt(2.0 * C))).astype(jnp.bfloat16)
    return (left_out, right_out)

def odd_bond(pair_in):
    right_one, left_next = pair_in
    rows_view = right_one.reshape(2 * K, C)
    cols_view = left_next.reshape(C, 2 * K)
    result = jnp.dot(rows_view.astype(jnp.float32), cols_view.astype(jnp.float32), preferred_element_type=jnp.float32) * (1.0 / math.sqrt(1.0 * C))
    return result.astype(jnp.bfloat16)

def reference(left_site, right_site, gate, omega):
    lefts = left_site.reshape(BONDS, 2 * C, C)
    rights = right_site.reshape(BONDS, C, 2 * C)
    left_out, right_out = lax.map(lambda pair_in: one_bond(pair_in, gate, omega), (lefts, rights))
    shifted = jnp.concatenate([left_out[1:], jnp.zeros((1, 2 * C, K), jnp.bfloat16)], axis=0)
    odd_pair = lax.map(odd_bond, (right_out, shifted))
    return (left_out.reshape(BONDS * 2 * C, K), right_out.reshape(BONDS * K, 2 * C), odd_pair.reshape(BONDS * 2 * K, 2 * K))
```

```python
import functools
import math

import jax
import jax.numpy as jnp
from jax import lax
from jax.experimental import pallas as pl
from jax.experimental.pallas import tpu as pltpu
from jax.sharding import PartitionSpec as P

LANES = 128
SUB = 8
TILE = 256
PARTS = 2
CHUNKS = 8
MESH = pl.DeviceIdType.MESH
F32 = jnp.float32
BF16 = jnp.bfloat16


def partner(me, distance):
    span = 2 * distance
    return lax.div(me, span) * span + lax.rem(lax.rem(me, span) + distance, span)


def distances(n):
    found = []
    while n > 1:
        n //= 2
        found.append(n)
    return found


def split(x):
    high = x.astype(BF16)
    return high, (x - high.astype(F32)).astype(BF16)


def dot(a, b):
    return jnp.dot(a, b, preferred_element_type=F32)


def inverse_factor(block):
    groups = LANES // SUB
    lane = lax.broadcasted_iota(jnp.int32, (SUB, LANES), 1)
    sub = lax.broadcasted_iota(jnp.int32, (SUB, LANES), 0)
    left = [block[g * SUB:(g + 1) * SUB, :] for g in range(groups)]
    right = [jnp.where(lane == sub + g * SUB, 1.0, 0.0) for g in range(groups)]
    rows = []

    def over_lanes(x, column):
        return jnp.broadcast_to(x[:, column:column + 1], (SUB, LANES))

    def over_rows(x, row):
        return jnp.broadcast_to(x[row:row + 1, :], (SUB, LANES))

    for g in range(groups):
        a, e = left[g], right[g]
        cols = [over_lanes(a, g * SUB + c) for c in range(SUB)]
        finished = jnp.zeros_like(e)
        for k in range(SUB):
            here = sub == k
            root = lax.rsqrt(over_rows(cols[k], k))
            inverse = root * root
            factor = cols[k] * inverse
            row_a, row_e = over_rows(a, k), over_rows(e, k)
            finished = jnp.where(here, row_e * root, finished)
            a = jnp.where(here, row_a * inverse, a - factor * row_a)
            e = jnp.where(here, row_e * inverse, e - factor * row_e)
            for c in range(k + 1, SUB):
                row_c = over_rows(cols[c], k)
                cols[c] = jnp.where(here, row_c * inverse, cols[c] - factor * row_c)
        rows.append(finished)
        if g + 1 == groups:
            break
        wide_a = [over_rows(a, k) for k in range(SUB)]
        wide_e = [over_rows(e, k) for k in range(SUB)]
        for i in range(g + 1, groups):
            coeff = [over_lanes(left[i], g * SUB + c) for c in range(SUB)]
            for c in range(SUB):
                left[i] = left[i] - coeff[c] * wide_a[c]
                right[i] = right[i] - coeff[c] * wide_e[c]
    return jnp.concatenate(rows, axis=0)


def layer_kernel(
    n, bonds, gate_ref, a_ref, b_ref, omega_ref, left_ref, right_ref, odd_ref,
    a_all, b_all, omega_all, theta, w_row, w_tall, work, gram_own, gram_in, panel, wide,
    flat, ahead, right_out, right_in, right_own, right_view, trace_own, trace_in,
    omega_send, omega_recv, b_send, b_recv, a_send, a_recv, gram_send, gram_recv, trace_send, trace_recv,
    shift_send, shift_recv, far_send, far_recv, near_send, near_recv, right_send, right_recv,
):
    bond, me = lax.axis_index("bond"), lax.axis_index("row")
    last = bonds - 1
    slots = n // 2
    slot, parity = lax.div(me, 2), lax.rem(me, 2)
    near = partner(me, 1)
    bond_dim = a_ref.shape[2]
    rank = omega_ref.shape[1]
    part_rows = a_ref.shape[1]
    block_rows = PARTS * part_rows
    half = block_rows // 2
    own_rank = rank // n
    blocks = rank // LANES
    depth = b_ref.shape[0]
    piece = depth // CHUNKS
    drawn = omega_ref.shape[0]

    def peer(j):
        return 2 * lax.rem(slot + j, slots) + parity

    def source(j, side):
        return 2 * lax.rem(slot + slots - j, slots) + side

    row_steps, bond_steps = distances(n), distances(bonds)

    barrier = pltpu.get_barrier_semaphore()
    greeted = 0
    for j in range(1, n):
        to = lax.rem(me + j, n)
        pl.semaphore_signal(barrier, inc=1, device_id={"row": to}, device_id_type=MESH)
        greeted += 1
    for s in bond_steps:
        pl.semaphore_signal(barrier, inc=1, device_id={"bond": partner(bond, s)}, device_id_type=MESH)
        greeted += 1
    for way in (1, last):
        to = lax.rem(bond + way, bonds)
        pl.semaphore_signal(barrier, inc=1, device_id={"bond": to}, device_id_type=MESH)
        greeted += 1
    pl.semaphore_wait(barrier, greeted)

    hops = [("row", s) for s in row_steps[:-1]] + [("bond", s) for s in bond_steps] + [("row", 1)]
    bits = [1 << (len(hops) - 1 - i) for i in range(len(hops))]
    hop_of = dict(zip(bits, hops))

    def whose(mask):
        at = {"row": me, "bond": bond}
        for bit in bits:
            if mask & bit:
                axis, s = hop_of[bit]
                at[axis] = partner(at[axis], s)
        return at["bond"] * n + at["row"]

    def omega_slot(mask):
        return omega_all.at[pl.ds(pl.multiple_of(whose(mask) * drawn, drawn), drawn), :]

    def omega_copy(mask, bit):
        axis, s = hop_of[bit]
        to = partner(me if axis == "row" else bond, s)
        return pltpu.make_async_remote_copy(
            src_ref=omega_slot(mask) if mask else omega_ref,
            dst_ref=omega_slot(mask),
            send_sem=omega_send.at[mask + bit],
            recv_sem=omega_recv.at[mask + bit],
            device_id={axis: to},
            device_id_type=MESH,
        )

    def lower_bits(mask):
        return [bit for bit in bits if mask == 0 or bit < (mask & -mask)]

    omega_order = [m for bit in bits for m in range(bit, 2 * bits[0], 2 * bit)]

    def b_copy(mask, s, k):
        at = me
        for step in row_steps:
            if mask & step:
                at = partner(at, step)
        start = pl.multiple_of(at * depth + k * piece, piece)
        target = b_all.at[pl.ds(start, piece), :]
        return pltpu.make_async_remote_copy(
            src_ref=target if mask else b_ref.at[k * piece:(k + 1) * piece, :],
            dst_ref=target,
            send_sem=b_send.at[mask + s, k],
            recv_sem=b_recv.at[mask + s, k],
            device_id={"row": partner(me, s)},
            device_id_type=MESH,
        )

    def b_lower(mask):
        return [s for s in row_steps if mask == 0 or s < (mask & -mask)]

    b_order = [m for s in row_steps for m in range(s, n, 2 * s)]

    def a_copy(j, q):
        return pltpu.make_async_remote_copy(
            src_ref=a_ref.at[q],
            dst_ref=a_all.at[slot, q],
            send_sem=a_send.at[j, q],
            recv_sem=a_recv.at[j, q],
            device_id={"row": peer(j)},
            device_id_type=MESH,
        )

    def a_arrival(j, q):
        return pltpu.make_async_remote_copy(
            src_ref=a_ref.at[q],
            dst_ref=a_all.at[lax.rem(slot + slots - j, slots), q],
            send_sem=a_send.at[j, q],
            recv_sem=a_recv.at[j, q],
            device_id={"row": peer(j)},
            device_id_type=MESH,
        )

    for bit in bits:
        omega_copy(0, bit).start()
    for s in row_steps:
        for k in range(CHUNKS):
            b_copy(0, s, k).start()
    for j in range(1, slots):
        for q in range(PARTS):
            a_copy(j, q).start()

    a_all[slot] = a_ref[...]
    b_all[pl.ds(pl.multiple_of(me * depth, depth), depth), :] = b_ref[...]
    omega_all[pl.ds(pl.multiple_of((bond * n + me) * drawn, drawn), drawn), :] = omega_ref[...]

    def clear(i, carry):
        at = pl.ds(pl.multiple_of(i * LANES, LANES), LANES)
        work[at, :] = jnp.zeros((LANES, rank), F32)
        gram_own[at, :] = jnp.zeros((LANES, rank), F32)
        return carry

    lax.fori_loop(0, blocks, clear, 0)

    todo = [(m, k) for m in b_order for k in range(CHUNKS)]
    every = -(-len(omega_order) // len(todo))
    steps = []
    for i, (m, k) in enumerate(todo):
        steps += [("o", o) for o in omega_order[i * every:(i + 1) * every]]
        steps.append(("b", (m, k)))
    for kind, what in steps:
        if kind == "o":
            low = what & -what
            omega_copy(what - low, low).wait_recv()
            for bit in lower_bits(what):
                omega_copy(what, bit).start()
        else:
            m, k = what
            b_copy(m - (m & -m), m & -m, k).wait_recv()
            for s in b_lower(m):
                b_copy(m, s, k).start()

    def mix(index, carry):
        j, q = lax.div(index, PARTS), lax.rem(index, PARTS)
        at = lax.rem(slot + slots - j, slots)

        @pl.when(j > 0)
        def _():
            a_arrival(j, q).wait_recv()

        base = pl.multiple_of((at * PARTS + q) * part_rows, part_rows)
        rows = pl.ds(base, part_rows)
        side = part_rows // 2

        def columns(cb, carry):
            c0 = pl.multiple_of(cb * TILE, TILE)
            c1 = pl.multiple_of(bond_dim + cb * TILE, TILE)
            block = a_all[at, q]
            product = [dot(block, b_all[:, pl.ds(c, TILE)]) for c in (c0, c1)]
            for s in range(2):
                for t in range(2):
                    total = None
                    for u in range(2):
                        for v in range(2):
                            term = gate_ref[2 * s + t, 2 * u + v] * product[v][u * side:(u + 1) * side, :]
                            total = term if total is None else total + term
                    theta[pl.ds(pl.multiple_of(base + s * side, side), side), pl.ds((c0, c1)[t], TILE)] = total.astype(BF16)
            return carry

        lax.fori_loop(0, bond_dim // TILE, columns, 0)

        def sketch(rb, carry):
            at_rank = pl.ds(pl.multiple_of(rb * TILE, TILE), TILE)
            value = dot(theta[rows, :], omega_all[:, at_rank].astype(BF16))
            w_row[rows, at_rank] = value.astype(BF16)
            w_tall[at_rank, rows] = value.T.astype(BF16)
            return carry

        lax.fori_loop(0, rank // TILE, sketch, 0)
        for i in range(rank // TILE):
            mine = slice(i * TILE, (i + 1) * TILE)
            gram_own[mine, i * TILE:] += dot(w_tall[mine, rows], w_row[rows, i * TILE:])
        return carry

    lax.fori_loop(0, slots * PARTS, mix, 0)

    def gram_copy(i):
        at = pl.ds(pl.multiple_of(i * LANES, LANES), LANES)
        return pltpu.make_async_remote_copy(
            src_ref=gram_own.at[at, :],
            dst_ref=gram_in.at[at, :],
            send_sem=gram_send.at[i],
            recv_sem=gram_recv.at[i],
            device_id={"row": near},
            device_id_type=MESH,
        )

    trace_copy = pltpu.make_async_remote_copy(
        src_ref=trace_own,
        dst_ref=trace_in,
        send_sem=trace_send,
        recv_sem=trace_recv,
        device_id={"row": near},
        device_id_type=MESH,
    )
    for i in range(blocks):
        gram_copy(i).start()
    eye = (
        lax.broadcasted_iota(jnp.int32, (LANES, LANES), 0)
        == lax.broadcasted_iota(jnp.int32, (LANES, LANES), 1)
    )
    column = lax.broadcasted_iota(jnp.int32, (LANES, rank), 1)
    total = jnp.zeros((LANES, LANES), F32)
    for d in range(blocks):
        at = slice(d * LANES, (d + 1) * LANES)
        total = total + jnp.where(eye, gram_own[at, at], 0.0)
    trace_own[...] = jnp.broadcast_to(jnp.sum(total, keepdims=True), (SUB, LANES))
    trace_copy.start()
    scale = 1.0 / (2.0 * bond_dim)
    trace_copy.wait()
    ridge = (trace_own[0:1, 0:1] + trace_in[0:1, 0:1]) * (scale * 0.01 / rank)

    def ahead_at(d, who):
        return ahead.at[d, :, pl.ds(pl.multiple_of(who * half, half), half), :]

    def shift_copy(d):
        return pltpu.make_async_remote_copy(
            src_ref=left_ref.at[d],
            dst_ref=ahead_at(d, me),
            send_sem=shift_send.at[d],
            recv_sem=shift_recv.at[d],
            device_id={"bond": lax.max(bond - 1, 0)},
            device_id_type=MESH,
        )

    def far_copy(j, d):
        return pltpu.make_async_remote_copy(
            src_ref=ahead_at(d, me),
            dst_ref=ahead_at(d, me),
            send_sem=far_send.at[j, d],
            recv_sem=far_recv.at[j, d],
            device_id={"row": peer(j)},
            device_id_type=MESH,
        )

    def far_arrival(j, d):
        return pltpu.make_async_remote_copy(
            src_ref=ahead_at(d, me),
            dst_ref=ahead_at(d, source(j, parity)),
            send_sem=far_send.at[j, d],
            recv_sem=far_recv.at[j, d],
            device_id={"row": peer(j)},
            device_id_type=MESH,
        )

    def near_copy(j, d, side):
        return pltpu.make_async_remote_copy(
            src_ref=ahead_at(d, source(j, side)),
            dst_ref=ahead_at(d, source(j, side)),
            send_sem=near_send.at[j, d],
            recv_sem=near_recv.at[j, d],
            device_id={"row": near},
            device_id_type=MESH,
        )

    def pass_on(d):
        shift_copy(d).wait_recv()
        for j in range(1, slots):
            far_copy(j, d).start()
        near_copy(0, d, parity).start()

    def pass_near(d):
        for j in range(1, slots):
            far_arrival(j, d).wait_recv()
            near_copy(j, d, parity).start()

    def eliminate(d, carry):
        start = pl.multiple_of(d * LANES, LANES)
        here = pl.ds(start, LANES)
        gram_copy(d).wait()
        panel[...] = work[here, :] + jnp.where(
            column >= start, (gram_own[here, :] + gram_in[here, :]) * scale, 0.0
        )
        inverse = inverse_factor(panel[:, here] + jnp.where(eye, ridge, 0.0))
        high, low = split(inverse)
        factor = jnp.concatenate([high, high, low], axis=1)
        high, low = split(panel[...])
        panel[...] = dot(factor, jnp.concatenate([high, low, high], axis=0))
        panel[:, here] = inverse
        high, low = split(panel[...])
        wide[0:LANES, :] = high
        wide[LANES:2 * LANES, :] = low
        wide[2 * LANES:, :] = high

        def update(i, carry):
            at = pl.multiple_of(i * LANES, LANES)
            there = pl.ds(at, LANES)
            high, low = split(panel[:, there].T)
            lower = jnp.concatenate([high, high, low], axis=1)
            kept = jnp.where((column >= start) & (column < start + LANES), 0.0, work[there, :])
            work[there, :] = kept - dot(lower, wide[...])
            return carry

        lax.fori_loop(d + 1, blocks, update, 0)

        known = column < start + LANES
        zero = jnp.zeros((LANES, rank), BF16)
        stacked = jnp.concatenate(
            [jnp.where(known, wide[0:LANES, :], zero), jnp.where(known, wide[LANES:2 * LANES, :], zero)], axis=0
        )
        both = dot(stacked, w_tall[...])
        basis = both[:LANES, :] + both[LANES:, :]
        flat[here, :] = basis.astype(BF16)
        side = part_rows // 2
        for q in range(PARTS):
            for s in range(2):
                first = pl.multiple_of(slot * block_rows + q * part_rows + s * side, side)
                left_ref[d, s, q * side:(q + 1) * side, :] = flat[here, pl.ds(first, side)].T

        @pl.when(bond > 0)
        def _():
            shift_copy(d).start()

        @pl.when((bond < last) & (d > 0))
        def _():
            pass_on(d - 1)

        @pl.when((bond < last) & (d > 1))
        def _():
            pass_near(d - 2)

        return carry

    lax.fori_loop(0, blocks, eliminate, 0)

    right_copy = pltpu.make_async_remote_copy(
        src_ref=right_out,
        dst_ref=right_in,
        send_sem=right_send,
        recv_sem=right_recv,
        device_id={"row": near},
        device_id_type=MESH,
    )

    def project(who, target):
        ranks = pl.ds(pl.multiple_of(who * own_rank, own_rank), own_rank)

        def columns(cb, carry):
            at = pl.ds(pl.multiple_of(cb * TILE, TILE), TILE)
            target[:, at] = dot(flat[ranks, :], theta[:, at]).astype(target.dtype)
            return carry

        lax.fori_loop(0, 2 * bond_dim // TILE, columns, 0)

    project(near, right_out)
    right_copy.start()
    project(me, right_own)

    @pl.when(bond < last)
    def _():
        if blocks > 1:
            pass_near(blocks - 2)
        pass_on(blocks - 1)

    right_copy.wait()
    right_scale = 1.0 / math.sqrt(2.0 * bond_dim)
    right_ref[...] = ((right_own[...] + right_in[...].astype(F32)) * right_scale).astype(BF16)

    @pl.when(bond < last)
    def _():
        view_rows = 2 * own_rank
        row = lax.broadcasted_iota(jnp.int32, (view_rows, view_rows), 0)
        col = lax.broadcasted_iota(jnp.int32, (view_rows, view_rows), 1)
        order = jnp.where(col == lax.div(row, 2) + lax.rem(row, 2) * own_rank, 1.0, 0.0).astype(BF16)
        stacked = jnp.concatenate([right_ref[:, :bond_dim], right_ref[:, bond_dim:]], axis=0)
        right_view[...] = dot(order, stacked).astype(BF16)
        odd_scale = 1.0 / math.sqrt(1.0 * bond_dim)

        def pair(d):
            for j in range(slots):
                near_copy(j, d, 1 - parity).wait_recv()
            both = jnp.concatenate([ahead[d, 0], ahead[d, 1]], axis=1)
            value = (dot(right_view[...], both) * odd_scale).astype(BF16)
            odd_ref[:, pl.ds(pl.multiple_of(d * LANES, LANES), LANES)] = value[:, :LANES]
            odd_ref[:, pl.ds(pl.multiple_of(rank + d * LANES, LANES), LANES)] = value[:, LANES:]

        def pairs(d, carry):
            pair(d)
            return carry

        lax.fori_loop(0, blocks - 1, pairs, 0)
        pass_near(blocks - 1)
        pair(blocks - 1)

        def sent(d, carry):
            for j in range(1, slots):
                far_copy(j, d).wait_send()
            for j in range(slots):
                near_copy(j, d, parity).wait_send()
            return carry

        lax.fori_loop(0, blocks, sent, 0)

    @pl.when(bond == last)
    def _():
        odd_ref[...] = jnp.zeros_like(odd_ref)

    @pl.when(bond > 0)
    def _():
        def sent(d, carry):
            shift_copy(d).wait_send()
            return carry

        lax.fori_loop(0, blocks, sent, 0)

    for mask in [0] + omega_order:
        for bit in lower_bits(mask):
            omega_copy(mask, bit).wait_send()
    for mask in [0] + b_order:
        for s in b_lower(mask):
            for k in range(CHUNKS):
                b_copy(mask, s, k).wait_send()
    for j in range(1, slots):
        for q in range(PARTS):
            a_copy(j, q).wait_send()


def layer(gate, left_parts, right_site, omega, n, bonds):
    parts, part_rows, bond_dim = left_parts.shape
    depth = right_site.shape[0]
    drawn, rank = omega.shape
    slots = n // 2
    block_rows = parts * part_rows
    rows = slots * block_rows
    half = block_rows // 2
    own_rank = rank // n
    blocks = rank // LANES
    dma = pltpu.SemaphoreType.DMA
    return pl.pallas_call(
        functools.partial(layer_kernel, n, bonds),
        out_shape=(
            jax.ShapeDtypeStruct((blocks, 2, half, LANES), BF16),
            jax.ShapeDtypeStruct((own_rank, 2 * bond_dim), BF16),
            jax.ShapeDtypeStruct((2 * own_rank, 2 * rank), BF16),
        ),
        in_specs=[pl.BlockSpec(memory_space=pltpu.SMEM)] + [pl.BlockSpec(memory_space=pltpu.VMEM)] * 3,
        out_specs=(pl.BlockSpec(memory_space=pltpu.VMEM),) * 3,
        scratch_shapes=[
            pltpu.VMEM((slots, parts, part_rows, bond_dim), BF16),
            pltpu.VMEM((n * depth, 2 * bond_dim), BF16),
            pltpu.VMEM((bonds * n * drawn, rank), omega.dtype),
            pltpu.VMEM((rows, 2 * bond_dim), BF16),
            pltpu.VMEM((rows, rank), BF16),
            pltpu.VMEM((rank, rows), BF16),
            pltpu.VMEM((rank, rank), F32),
            pltpu.VMEM((rank, rank), F32),
            pltpu.VMEM((rank, rank), F32),
            pltpu.VMEM((LANES, rank), F32),
            pltpu.VMEM((3 * LANES, rank), BF16),
            pltpu.VMEM((rank, rows), BF16),
            pltpu.VMEM((blocks, 2, n * half, LANES), BF16),
            pltpu.VMEM((own_rank, 2 * bond_dim), BF16),
            pltpu.VMEM((own_rank, 2 * bond_dim), BF16),
            pltpu.VMEM((own_rank, 2 * bond_dim), F32),
            pltpu.VMEM((2 * own_rank, bond_dim), BF16),
            pltpu.VMEM((SUB, LANES), F32),
            pltpu.VMEM((SUB, LANES), F32),
            dma((bonds * n,)), dma((bonds * n,)),
            dma((n, CHUNKS)), dma((n, CHUNKS)),
            dma((slots, parts)), dma((slots, parts)),
            dma((blocks,)), dma((blocks,)),
            dma, dma,
            dma((blocks,)), dma((blocks,)),
            dma((slots, blocks)), dma((slots, blocks)),
            dma((slots, blocks)), dma((slots, blocks)),
            dma, dma,
        ],
        compiler_params=pltpu.CompilerParams(
            collective_id=0, has_side_effects=True, vmem_limit_bytes=62 * 1024 * 1024
        ),
        name="layer",
    )(gate, left_parts, right_site, omega)


def shards(left_site, right_site, gate, omega):
    n, bonds = lax.axis_size("row"), lax.axis_size("bond")
    rows, bond_dim = left_site.shape
    rank = omega.shape[1]
    per = rows // (2 * PARTS)
    left_parts = left_site.reshape(PARTS, per, 2, bond_dim).transpose(0, 2, 1, 3).reshape(PARTS, 2 * per, bond_dim)
    if omega.shape[0] % 16:
        omega = omega.astype(F32)
    left_blocks, right_new, odd_pair = layer(gate, left_parts, right_site, omega, n, bonds)
    left_new = left_blocks.transpose(2, 1, 0, 3).reshape(rows, rank)
    return (left_new, right_new, odd_pair)


def solution(mesh):
    split_rows = P(("bond", "row"), None)
    return jax.shard_map(
        shards,
        mesh=mesh,
        in_specs=(split_rows, split_rows, P(), split_rows),
        out_specs=(split_rows, split_rows, split_rows),
        check_vma=False,
    )
```

```python
import functools
import math

import jax
import jax.numpy as jnp
from jax import lax
from jax.experimental import pallas as pl
from jax.experimental.pallas import tpu as pltpu
from jax.sharding import PartitionSpec as P

LANES = 128
SUB = 8
TILE = 256
PARTS = 2
CHUNKS = 8
MESH = pl.DeviceIdType.MESH
F32 = jnp.float32
BF16 = jnp.bfloat16


def partner(me, distance):
    span = 2 * distance
    return lax.div(me, span) * span + lax.rem(lax.rem(me, span) + distance, span)


def distances(n):
    found = []
    while n > 1:
        n //= 2
        found.append(n)
    return found


def split(x):
    high = x.astype(BF16)
    return high, (x - high.astype(F32)).astype(BF16)


def dot(a, b):
    return jnp.dot(a, b, preferred_element_type=F32)


def inverse_factor(block):
    groups = LANES // SUB
    lane = lax.broadcasted_iota(jnp.int32, (SUB, LANES), 1)
    sub = lax.broadcasted_iota(jnp.int32, (SUB, LANES), 0)
    left = [block[g * SUB:(g + 1) * SUB, :] for g in range(groups)]
    right = [jnp.where(lane == sub + g * SUB, 1.0, 0.0) for g in range(groups)]
    rows = []

    def over_lanes(x, column):
        return jnp.broadcast_to(x[:, column:column + 1], (SUB, LANES))

    def over_rows(x, row):
        return jnp.broadcast_to(x[row:row + 1, :], (SUB, LANES))

    for g in range(groups):
        a, e = left[g], right[g]
        cols = [over_lanes(a, g * SUB + c) for c in range(SUB)]
        finished = jnp.zeros_like(e)
        for k in range(SUB):
            here = sub == k
            root = lax.rsqrt(over_rows(cols[k], k))
            inverse = root * root
            factor = cols[k] * inverse
            row_a, row_e = over_rows(a, k), over_rows(e, k)
            finished = jnp.where(here, row_e * root, finished)
            a = jnp.where(here, row_a * inverse, a - factor * row_a)
            e = jnp.where(here, row_e * inverse, e - factor * row_e)
            for c in range(k + 1, SUB):
                row_c = over_rows(cols[c], k)
                cols[c] = jnp.where(here, row_c * inverse, cols[c] - factor * row_c)
        rows.append(finished)
        if g + 1 == groups:
            break
        wide_a = [over_rows(a, k) for k in range(SUB)]
        wide_e = [over_rows(e, k) for k in range(SUB)]
        for i in range(g + 1, groups):
            coeff = [over_lanes(left[i], g * SUB + c) for c in range(SUB)]
            for c in range(SUB):
                left[i] = left[i] - coeff[c] * wide_a[c]
                right[i] = right[i] - coeff[c] * wide_e[c]
    return jnp.concatenate(rows, axis=0)


def by_spin(rows):
    row = lax.broadcasted_iota(jnp.int32, (rows, rows), 0)
    col = lax.broadcasted_iota(jnp.int32, (rows, rows), 1)
    side = rows // 2
    return jnp.where(col == 2 * lax.rem(row, side) + lax.div(row, side), 1.0, 0.0).astype(BF16)


def interleave(rows):
    row = lax.broadcasted_iota(jnp.int32, (rows, rows), 0)
    col = lax.broadcasted_iota(jnp.int32, (rows, rows), 1)
    side = rows // 2
    return jnp.where(col == lax.div(row, 2) + lax.rem(row, 2) * side, 1.0, 0.0).astype(BF16)


def layer_kernel(
    n, bonds, gate_ref, a_ref, b_ref, omega_ref, left_out, right_ref, odd_ref,
    a_all, a_turned, b_all, omega_all, theta, w_row, w_tall, high_all, low_all, gram_own, gram_in,
    diagonal, pending, factor, coeff, flat, left_ref, ahead, right_out, right_in, right_own, right_view, trace_own, trace_in,
    omega_send, omega_recv, b_send, b_recv, a_send, a_recv, gram_send, gram_recv, trace_send, trace_recv,
    shift_send, shift_recv, far_send, far_recv, near_send, near_recv, right_send, right_recv,
):
    bond, me = lax.axis_index("bond"), lax.axis_index("row")
    last = bonds - 1
    slots = n // 2
    slot, parity = lax.div(me, 2), lax.rem(me, 2)
    near = partner(me, 1)
    bond_dim = a_ref.shape[1]
    rank = omega_ref.shape[1]
    block_rows = a_ref.shape[0]
    part_rows = block_rows // PARTS
    half = block_rows // 2
    own_rank = rank // n
    blocks = rank // LANES
    depth = b_ref.shape[0]
    piece = depth // CHUNKS
    drawn = omega_ref.shape[0]

    def peer(j):
        return 2 * lax.rem(slot + j, slots) + parity

    def source(j, side):
        return 2 * lax.rem(slot + slots - j, slots) + side

    row_steps, bond_steps = distances(n), distances(bonds)

    barrier = pltpu.get_barrier_semaphore()
    greeted = 0
    for j in range(1, n):
        to = lax.rem(me + j, n)
        pl.semaphore_signal(barrier, inc=1, device_id={"row": to}, device_id_type=MESH)
        greeted += 1
    for s in bond_steps:
        pl.semaphore_signal(barrier, inc=1, device_id={"bond": partner(bond, s)}, device_id_type=MESH)
        greeted += 1
    for way in (1, last):
        to = lax.rem(bond + way, bonds)
        pl.semaphore_signal(barrier, inc=1, device_id={"bond": to}, device_id_type=MESH)
        greeted += 1
    pl.semaphore_wait(barrier, greeted)

    hops = [("row", s) for s in row_steps[:-1]] + [("bond", s) for s in bond_steps] + [("row", 1)]
    bits = [1 << (len(hops) - 1 - i) for i in range(len(hops))]
    hop_of = dict(zip(bits, hops))

    def whose(mask):
        at = {"row": me, "bond": bond}
        for bit in bits:
            if mask & bit:
                axis, s = hop_of[bit]
                at[axis] = partner(at[axis], s)
        return at["bond"] * n + at["row"]

    def omega_slot(mask):
        return omega_all.at[pl.ds(pl.multiple_of(whose(mask) * drawn, drawn), drawn), :]

    def omega_copy(mask, bit):
        axis, s = hop_of[bit]
        to = partner(me if axis == "row" else bond, s)
        return pltpu.make_async_remote_copy(
            src_ref=omega_slot(mask) if mask else omega_ref,
            dst_ref=omega_slot(mask),
            send_sem=omega_send.at[mask + bit],
            recv_sem=omega_recv.at[mask + bit],
            device_id={axis: to},
            device_id_type=MESH,
        )

    def lower_bits(mask):
        return [bit for bit in bits if mask == 0 or bit < (mask & -mask)]

    omega_order = [m for bit in bits for m in range(bit, 2 * bits[0], 2 * bit)]

    def b_copy(mask, s, k):
        at = me
        for step in row_steps:
            if mask & step:
                at = partner(at, step)
        start = pl.multiple_of(at * depth + k * piece, piece)
        target = b_all.at[pl.ds(start, piece), :]
        return pltpu.make_async_remote_copy(
            src_ref=target if mask else b_ref.at[k * piece:(k + 1) * piece, :],
            dst_ref=target,
            send_sem=b_send.at[mask + s, k],
            recv_sem=b_recv.at[mask + s, k],
            device_id={"row": partner(me, s)},
            device_id_type=MESH,
        )

    def b_lower(mask):
        return [s for s in row_steps if mask == 0 or s < (mask & -mask)]

    b_order = [m for s in row_steps for m in range(s, n, 2 * s)]

    def a_copy(j, q):
        return pltpu.make_async_remote_copy(
            src_ref=a_ref.at[pl.ds(pl.multiple_of(q * part_rows, part_rows), part_rows), :],
            dst_ref=a_all.at[slot, q],
            send_sem=a_send.at[j, q],
            recv_sem=a_recv.at[j, q],
            device_id={"row": peer(j)},
            device_id_type=MESH,
        )

    def a_arrival(j, q):
        return pltpu.make_async_remote_copy(
            src_ref=a_ref.at[pl.ds(pl.multiple_of(q * part_rows, part_rows), part_rows), :],
            dst_ref=a_all.at[lax.rem(slot + slots - j, slots), q],
            send_sem=a_send.at[j, q],
            recv_sem=a_recv.at[j, q],
            device_id={"row": peer(j)},
            device_id_type=MESH,
        )

    for bit in bits:
        omega_copy(0, bit).start()
    for s in row_steps:
        for k in range(CHUNKS):
            b_copy(0, s, k).start()
    for j in range(1, slots):
        for q in range(PARTS):
            a_copy(j, q).start()

    for q in range(PARTS):
        a_all[slot, q] = a_ref[q * part_rows:(q + 1) * part_rows, :]
    b_all[pl.ds(pl.multiple_of(me * depth, depth), depth), :] = b_ref[...]
    omega_all[pl.ds(pl.multiple_of((bond * n + me) * drawn, drawn), drawn), :] = omega_ref[...]

    def clear(i, carry):
        at = pl.ds(pl.multiple_of(i * LANES, LANES), LANES)
        high_all[at, :] = jnp.zeros((LANES, rank), BF16)
        low_all[at, :] = jnp.zeros((LANES, rank), BF16)
        gram_own[at, :] = jnp.zeros((LANES, rank), F32)
        return carry

    lax.fori_loop(0, blocks, clear, 0)

    todo = [(m, k) for m in b_order for k in range(CHUNKS)]
    every = -(-len(omega_order) // len(todo))
    steps = []
    for i, (m, k) in enumerate(todo):
        steps += [("o", o) for o in omega_order[i * every:(i + 1) * every]]
        steps.append(("b", (m, k)))
    for kind, what in steps:
        if kind == "o":
            low = what & -what
            omega_copy(what - low, low).wait_recv()
            for bit in lower_bits(what):
                omega_copy(what, bit).start()
        else:
            m, k = what
            b_copy(m - (m & -m), m & -m, k).wait_recv()
            for s in b_lower(m):
                b_copy(m, s, k).start()

    def mix(index, carry):
        j, q = lax.div(index, PARTS), lax.rem(index, PARTS)
        at = lax.rem(slot + slots - j, slots)

        @pl.when(j > 0)
        def _():
            a_arrival(j, q).wait_recv()

        base = pl.multiple_of((at * PARTS + q) * part_rows, part_rows)
        rows = pl.ds(base, part_rows)
        side = part_rows // 2
        a_turned[...] = dot(by_spin(part_rows), a_all[at, q]).astype(BF16)

        def columns(cb, carry):
            c0 = pl.multiple_of(cb * TILE, TILE)
            c1 = pl.multiple_of(bond_dim + cb * TILE, TILE)
            product = [dot(a_turned[...], b_all[:, pl.ds(c, TILE)]) for c in (c0, c1)]
            for s in range(2):
                for t in range(2):
                    total = None
                    for u in range(2):
                        for v in range(2):
                            term = gate_ref[2 * s + t, 2 * u + v] * product[v][u * side:(u + 1) * side, :]
                            total = term if total is None else total + term
                    theta[pl.ds(pl.multiple_of(base + s * side, side), side), pl.ds((c0, c1)[t], TILE)] = total.astype(BF16)
            return carry

        lax.fori_loop(0, bond_dim // TILE, columns, 0)

        def sketch(rb, carry):
            at_rank = pl.ds(pl.multiple_of(rb * TILE, TILE), TILE)
            value = dot(theta[rows, :], omega_all[:, at_rank].astype(BF16))
            w_row[rows, at_rank] = value.astype(BF16)
            w_tall[at_rank, rows] = value.T.astype(BF16)
            return carry

        lax.fori_loop(0, rank // TILE, sketch, 0)
        for i in range(rank // TILE):
            mine = slice(i * TILE, (i + 1) * TILE)
            gram_own[mine, i * TILE:] += dot(w_tall[mine, rows], w_row[rows, i * TILE:])
        return carry

    lax.fori_loop(0, slots * PARTS, mix, 0)

    def gram_copy(i):
        at = pl.ds(pl.multiple_of(i * LANES, LANES), LANES)
        return pltpu.make_async_remote_copy(
            src_ref=gram_own.at[at, :],
            dst_ref=gram_in.at[at, :],
            send_sem=gram_send.at[i],
            recv_sem=gram_recv.at[i],
            device_id={"row": near},
            device_id_type=MESH,
        )

    trace_copy = pltpu.make_async_remote_copy(
        src_ref=trace_own,
        dst_ref=trace_in,
        send_sem=trace_send,
        recv_sem=trace_recv,
        device_id={"row": near},
        device_id_type=MESH,
    )
    for i in range(blocks):
        gram_copy(i).start()
    eye = (
        lax.broadcasted_iota(jnp.int32, (LANES, LANES), 0)
        == lax.broadcasted_iota(jnp.int32, (LANES, LANES), 1)
    )
    total = jnp.zeros((LANES, LANES), F32)
    for d in range(blocks):
        at = slice(d * LANES, (d + 1) * LANES)
        total = total + jnp.where(eye, gram_own[at, at], 0.0)
    trace_own[...] = jnp.broadcast_to(jnp.sum(total, keepdims=True), (SUB, LANES))
    trace_copy.start()
    scale = 1.0 / (2.0 * bond_dim)
    trace_copy.wait()
    ridge = (trace_own[0:1, 0:1] + trace_in[0:1, 0:1]) * (scale * 0.01 / rank)

    def ahead_at(d, who):
        return ahead.at[d, :, pl.ds(pl.multiple_of(who * half, half), half), :]

    def shift_copy(d):
        return pltpu.make_async_remote_copy(
            src_ref=left_ref.at[d],
            dst_ref=ahead_at(d, me),
            send_sem=shift_send.at[d],
            recv_sem=shift_recv.at[d],
            device_id={"bond": lax.max(bond - 1, 0)},
            device_id_type=MESH,
        )

    def far_copy(j, d):
        return pltpu.make_async_remote_copy(
            src_ref=ahead_at(d, me),
            dst_ref=ahead_at(d, me),
            send_sem=far_send.at[j, d],
            recv_sem=far_recv.at[j, d],
            device_id={"row": peer(j)},
            device_id_type=MESH,
        )

    def far_arrival(j, d):
        return pltpu.make_async_remote_copy(
            src_ref=ahead_at(d, me),
            dst_ref=ahead_at(d, source(j, parity)),
            send_sem=far_send.at[j, d],
            recv_sem=far_recv.at[j, d],
            device_id={"row": peer(j)},
            device_id_type=MESH,
        )

    def near_copy(j, d, side):
        return pltpu.make_async_remote_copy(
            src_ref=ahead_at(d, source(j, side)),
            dst_ref=ahead_at(d, source(j, side)),
            send_sem=near_send.at[j, d],
            recv_sem=near_recv.at[j, d],
            device_id={"row": near},
            device_id_type=MESH,
        )

    def pass_on(d):
        shift_copy(d).wait_recv()
        for j in range(1, slots):
            far_copy(j, d).start()
        near_copy(0, d, parity).start()

    def pass_near(d):
        for j in range(1, slots):
            far_arrival(j, d).wait_recv()
            near_copy(j, d, parity).start()

    column = lax.broadcasted_iota(jnp.int32, (LANES, rank), 1)
    tall_row = lax.broadcasted_iota(jnp.int32, (rank, LANES), 0)
    ones = jnp.where(eye, 1.0, 0.0)

    def three(x):
        high, low = split(x)
        return jnp.concatenate([high, low, high], axis=0)

    def finish(d):
        start = pl.multiple_of(d * LANES, LANES)
        here = pl.ds(start, LANES)
        rows = dot(factor[...], three(pending[...]))
        high_all[here, :], low_all[here, :] = split(rows)
        for ref in (high_all, low_all):
            ref[:, here] = jnp.where(tall_row < start, jnp.zeros((rank, LANES), BF16), ref[:, here])
        high, low = split(jnp.where(column < start + LANES, rows, 0.0))
        both = dot(jnp.concatenate([high, low], axis=0), w_tall[...])
        flat[here, :] = (both[:LANES, :] + both[LANES:, :]).astype(BF16)
        side = part_rows // 2
        for q in range(PARTS):
            for s in range(2):
                first = pl.multiple_of(slot * block_rows + q * part_rows + s * side, side)
                left_ref[d, s, q * side:(q + 1) * side, :] = flat[here, pl.ds(first, side)].T

    def eliminate(d, carry):
        start = pl.multiple_of(d * LANES, LANES)
        here = pl.ds(start, LANES)
        after = lax.min(d + 1, blocks - 1)
        there = pl.ds(pl.multiple_of(after * LANES, LANES), LANES)

        @pl.when(d + 1 < blocks)
        def _():
            gram_copy(d + 1).wait()

        inverse = inverse_factor(diagonal[...])
        finish(lax.max(d - 1, 0))

        known = dot(coeff[...], high_all[...])
        known = known[:LANES, :] + known[LANES:, :] + dot(coeff[:LANES, :], low_all[...])
        row = jnp.where(column >= start, (gram_own[here, :] + gram_in[here, :]) * scale, 0.0) - known
        pending[...] = row
        pending[:, here] = ones

        next_high, next_low = high_all[:, there], low_all[:, there]
        coeff[:LANES, :] = next_high.T
        coeff[LANES:, :] = next_low.T
        known = dot(coeff[...], next_high)
        known = known[:LANES, :] + known[LANES:, :] + dot(coeff[:LANES, :], next_low)
        ahead_block = (gram_own[there, there] + gram_in[there, there]) * scale - known + ones * ridge

        high, low = split(inverse)
        thrice = jnp.concatenate([high, high, low], axis=1)
        factor[...] = thrice
        solved = dot(thrice, three(pending[:, there]))
        high, low = split(solved.T)
        coeff[:LANES, here] = high
        coeff[LANES:, here] = low
        diagonal[...] = ahead_block - dot(jnp.concatenate([high, high, low], axis=1), three(solved))

        @pl.when((bond > 0) & (d > 0))
        def _():
            shift_copy(d - 1).start()

        @pl.when((bond < last) & (d > 1))
        def _():
            pass_on(d - 2)

        @pl.when((bond < last) & (d > 2))
        def _():
            pass_near(d - 3)

        return carry

    pending[...] = jnp.zeros_like(pending)
    factor[...] = jnp.zeros_like(factor)
    coeff[...] = jnp.zeros_like(coeff)
    gram_copy(0).wait()
    diagonal[...] = (gram_own[:LANES, :LANES] + gram_in[:LANES, :LANES]) * scale + ones * ridge
    lax.fori_loop(0, blocks, eliminate, 0)
    finish(blocks - 1)

    @pl.when(bond > 0)
    def _():
        shift_copy(blocks - 1).start()


    right_copy = pltpu.make_async_remote_copy(
        src_ref=right_out,
        dst_ref=right_in,
        send_sem=right_send,
        recv_sem=right_recv,
        device_id={"row": near},
        device_id_type=MESH,
    )

    def project(who, target):
        ranks = pl.ds(pl.multiple_of(who * own_rank, own_rank), own_rank)

        def columns(cb, carry):
            at = pl.ds(pl.multiple_of(cb * TILE, TILE), TILE)
            target[:, at] = dot(flat[ranks, :], theta[:, at]).astype(target.dtype)
            return carry

        lax.fori_loop(0, 2 * bond_dim // TILE, columns, 0)

    project(near, right_out)
    right_copy.start()
    project(me, right_own)

    @pl.when(bond < last)
    def _():
        pass_on(blocks - 2)
        pass_near(blocks - 3)

    turn = interleave(block_rows)
    for d in range(0, blocks, 2):
        pair_of = [jnp.concatenate([left_ref[d + i, 0], left_ref[d + i, 1]], axis=0) for i in range(2)]
        left_out[:, d * LANES:(d + 2) * LANES] = dot(turn, jnp.concatenate(pair_of, axis=1)).astype(BF16)

    @pl.when(bond < last)
    def _():
        pass_on(blocks - 1)
        pass_near(blocks - 2)

    right_copy.wait()
    right_scale = 1.0 / math.sqrt(2.0 * bond_dim)
    right_ref[...] = ((right_own[...] + right_in[...].astype(F32)) * right_scale).astype(BF16)

    @pl.when(bond < last)
    def _():
        stacked = jnp.concatenate([right_ref[:, :bond_dim], right_ref[:, bond_dim:]], axis=0)
        right_view[...] = dot(interleave(2 * own_rank), stacked).astype(BF16)
        odd_scale = 1.0 / math.sqrt(1.0 * bond_dim)

        def pair(d):
            for j in range(slots):
                near_copy(j, d, 1 - parity).wait_recv()
            both = jnp.concatenate([ahead[d, 0], ahead[d, 1]], axis=1)
            value = (dot(right_view[...], both) * odd_scale).astype(BF16)
            odd_ref[:, pl.ds(pl.multiple_of(d * LANES, LANES), LANES)] = value[:, :LANES]
            odd_ref[:, pl.ds(pl.multiple_of(rank + d * LANES, LANES), LANES)] = value[:, LANES:]

        def pairs(d, carry):
            pair(d)
            return carry

        lax.fori_loop(0, blocks - 1, pairs, 0)
        pass_near(blocks - 1)
        pair(blocks - 1)

        def sent(d, carry):
            for j in range(1, slots):
                far_copy(j, d).wait_send()
            for j in range(slots):
                near_copy(j, d, parity).wait_send()
            return carry

        lax.fori_loop(0, blocks, sent, 0)

    @pl.when(bond == last)
    def _():
        odd_ref[...] = jnp.zeros_like(odd_ref)

    @pl.when(bond > 0)
    def _():
        def sent(d, carry):
            shift_copy(d).wait_send()
            return carry

        lax.fori_loop(0, blocks, sent, 0)

    for mask in [0] + omega_order:
        for bit in lower_bits(mask):
            omega_copy(mask, bit).wait_send()
    for mask in [0] + b_order:
        for s in b_lower(mask):
            for k in range(CHUNKS):
                b_copy(mask, s, k).wait_send()
    for j in range(1, slots):
        for q in range(PARTS):
            a_copy(j, q).wait_send()


def layer(gate, left_site, right_site, omega, n, bonds):
    block_rows, bond_dim = left_site.shape
    part_rows = block_rows // PARTS
    depth = right_site.shape[0]
    drawn, rank = omega.shape
    slots = n // 2
    rows = slots * block_rows
    half = block_rows // 2
    own_rank = rank // n
    blocks = rank // LANES
    dma = pltpu.SemaphoreType.DMA
    return pl.pallas_call(
        functools.partial(layer_kernel, n, bonds),
        out_shape=(
            jax.ShapeDtypeStruct((block_rows, rank), BF16),
            jax.ShapeDtypeStruct((own_rank, 2 * bond_dim), BF16),
            jax.ShapeDtypeStruct((2 * own_rank, 2 * rank), BF16),
        ),
        in_specs=[pl.BlockSpec(memory_space=pltpu.SMEM)] + [pl.BlockSpec(memory_space=pltpu.VMEM)] * 3,
        out_specs=(pl.BlockSpec(memory_space=pltpu.VMEM),) * 3,
        scratch_shapes=[
            pltpu.VMEM((slots, PARTS, part_rows, bond_dim), BF16),
            pltpu.VMEM((part_rows, bond_dim), BF16),
            pltpu.VMEM((n * depth, 2 * bond_dim), BF16),
            pltpu.VMEM((bonds * n * drawn, rank), omega.dtype),
            pltpu.VMEM((rows, 2 * bond_dim), BF16),
            pltpu.VMEM((rows, rank), BF16),
            pltpu.VMEM((rank, rows), BF16),
            pltpu.VMEM((rank, rank), BF16),
            pltpu.VMEM((rank, rank), BF16),
            pltpu.VMEM((rank, rank), F32),
            pltpu.VMEM((rank, rank), F32),
            pltpu.VMEM((LANES, LANES), F32),
            pltpu.VMEM((LANES, rank), F32),
            pltpu.VMEM((LANES, 3 * LANES), BF16),
            pltpu.VMEM((2 * LANES, rank), BF16),
            pltpu.VMEM((rank, rows), BF16),
            pltpu.VMEM((blocks, 2, half, LANES), BF16),
            pltpu.VMEM((blocks, 2, n * half, LANES), BF16),
            pltpu.VMEM((own_rank, 2 * bond_dim), BF16),
            pltpu.VMEM((own_rank, 2 * bond_dim), BF16),
            pltpu.VMEM((own_rank, 2 * bond_dim), F32),
            pltpu.VMEM((2 * own_rank, bond_dim), BF16),
            pltpu.VMEM((SUB, LANES), F32),
            pltpu.VMEM((SUB, LANES), F32),
            dma((bonds * n,)), dma((bonds * n,)),
            dma((n, CHUNKS)), dma((n, CHUNKS)),
            dma((slots, PARTS)), dma((slots, PARTS)),
            dma((blocks,)), dma((blocks,)),
            dma, dma,
            dma((blocks,)), dma((blocks,)),
            dma((slots, blocks)), dma((slots, blocks)),
            dma((slots, blocks)), dma((slots, blocks)),
            dma, dma,
        ],
        compiler_params=pltpu.CompilerParams(
            collective_id=0, has_side_effects=True, vmem_limit_bytes=62 * 1024 * 1024
        ),
        name="layer",
    )(gate, left_site, right_site, omega)


def shards(left_site, right_site, gate, omega):
    n, bonds = lax.axis_size("row"), lax.axis_size("bond")
    if omega.shape[0] % 16:
        omega = omega.astype(F32)
    return layer(gate, left_site, right_site, omega, n, bonds)


def solution(mesh):
    split_rows = P(("bond", "row"), None)
    return jax.shard_map(
        shards,
        mesh=mesh,
        in_specs=(split_rows, split_rows, P(), split_rows),
        out_specs=(split_rows, split_rows, split_rows),
        check_vma=False,
    )
```

```python
import functools
import math

import jax
import jax.numpy as jnp
from jax import lax
from jax.experimental import pallas as pl
from jax.experimental.pallas import tpu as pltpu
from jax.sharding import PartitionSpec as P

LANES = 128
SUB = 8
TILE = 256
PARTS = 2
CHUNKS = 8
MESH = pl.DeviceIdType.MESH
F32 = jnp.float32
BF16 = jnp.bfloat16


def partner(me, distance):
    span = 2 * distance
    return lax.div(me, span) * span + lax.rem(lax.rem(me, span) + distance, span)


def distances(n):
    found = []
    while n > 1:
        n //= 2
        found.append(n)
    return found


def split(x):
    high = x.astype(BF16)
    return high, (x - high.astype(F32)).astype(BF16)


def dot(a, b):
    return jnp.dot(a, b, preferred_element_type=F32)


def inverse_factor(block):
    groups = LANES // SUB
    lane = lax.broadcasted_iota(jnp.int32, (SUB, LANES), 1)
    sub = lax.broadcasted_iota(jnp.int32, (SUB, LANES), 0)
    rows = [block[g * SUB:(g + 1) * SUB, :] for g in range(groups)]
    finished = []

    def over_lanes(x, column):
        return jnp.broadcast_to(x[:, column:column + 1], (SUB, LANES))

    def over_rows(x, row):
        return jnp.broadcast_to(x[row:row + 1, :], (SUB, LANES))

    def inside(g):
        return (lane >= g * SUB) & (lane < (g + 1) * SUB)

    def columns(x, g):
        return [over_lanes(x, g * SUB + c) for c in range(SUB)]

    def pivots(g, cols, low=None, after=None):
        x = jnp.where(inside(g), jnp.where(lane == sub + g * SUB, 1.0, 0.0), rows[g])
        out = jnp.zeros_like(x)
        for k in range(SUB):
            here = sub == k
            root = lax.rsqrt(over_rows(cols[k], k))
            inverse = root * root
            row = over_rows(x, k)
            out = jnp.where(here, row * root, out)
            ratio = cols[k] * inverse
            x = jnp.where(here, row * inverse, x - ratio * row)
            tops = {c: over_rows(cols[c], k) for c in range(k + 1, SUB)}
            for c in range(k + 1, SUB):
                cols[c] = jnp.where(here, tops[c] * inverse, cols[c] - ratio * tops[c])
            if low is not None:
                below = low[k] * inverse
                for c in range(SUB):
                    after[c] = after[c] - below * over_rows(low[k], c)
                for c in range(k + 1, SUB):
                    low[c] = low[c] - below * tops[c]
        finished.append(jnp.where(lane <= sub + g * SUB, out, 0.0))
        return [over_rows(x, k) for k in range(SUB)]

    def remove(i, g, coeff, wide):
        rest = jnp.where(inside(g), 0.0, rows[i])
        for c in range(SUB):
            rest = rest - coeff[c] * wide[c]
        rows[i] = rest

    for g in range(0, groups, 2):
        cols = columns(rows[g], g)
        low, after = columns(rows[g + 1], g), columns(rows[g + 1], g + 1)
        wide = pivots(g, cols, list(low), after)
        remove(g + 1, g, low, wide)
        for i in range(g + 2, groups):
            remove(i, g, columns(rows[i], g), wide)
        wide = pivots(g + 1, after)
        for i in range(g + 2, groups):
            remove(i, g + 1, columns(rows[i], g + 1), wide)
    return jnp.concatenate(finished, axis=0)


def by_spin(rows):
    row = lax.broadcasted_iota(jnp.int32, (rows, rows), 0)
    col = lax.broadcasted_iota(jnp.int32, (rows, rows), 1)
    side = rows // 2
    return jnp.where(col == 2 * lax.rem(row, side) + lax.div(row, side), 1.0, 0.0).astype(BF16)


def interleave(rows):
    row = lax.broadcasted_iota(jnp.int32, (rows, rows), 0)
    col = lax.broadcasted_iota(jnp.int32, (rows, rows), 1)
    side = rows // 2
    return jnp.where(col == lax.div(row, 2) + lax.rem(row, 2) * side, 1.0, 0.0).astype(BF16)


def layer_kernel(
    n, bonds, gate_ref, a_ref, b_ref, omega_ref, left_out, right_ref, odd_ref,
    a_all, a_turned, b_all, omega_all, theta, w_row, w_tall, high_all, low_all, gram_own, gram_in,
    diagonal, pending, factor, coeff, flat, left_ref, ahead, right_out, right_in, right_view, trace_own, trace_in,
    omega_send, omega_recv, b_send, b_recv, a_send, a_recv, gram_send, gram_recv, trace_send, trace_recv,
    shift_send, shift_recv, far_send, far_recv, near_send, near_recv, right_send, right_recv,
):
    bond, me = lax.axis_index("bond"), lax.axis_index("row")
    last = bonds - 1
    slots = n // 2
    slot, parity = lax.div(me, 2), lax.rem(me, 2)
    near = partner(me, 1)
    bond_dim = a_ref.shape[1]
    rank = omega_ref.shape[1]
    block_rows = a_ref.shape[0]
    part_rows = block_rows // PARTS
    half = block_rows // 2
    own_rank = rank // n
    blocks = rank // LANES
    depth = b_ref.shape[0]
    piece = depth // CHUNKS
    drawn = omega_ref.shape[0]

    def peer(j):
        return 2 * lax.rem(slot + j, slots) + parity

    def source(j, side):
        return 2 * lax.rem(slot + slots - j, slots) + side

    row_steps, bond_steps = distances(n), distances(bonds)

    barrier = pltpu.get_barrier_semaphore()
    greeted = 0
    for j in range(1, n):
        to = lax.rem(me + j, n)
        pl.semaphore_signal(barrier, inc=1, device_id={"row": to}, device_id_type=MESH)
        greeted += 1
    for s in bond_steps:
        pl.semaphore_signal(barrier, inc=1, device_id={"bond": partner(bond, s)}, device_id_type=MESH)
        greeted += 1
    for way in (1, last):
        to = lax.rem(bond + way, bonds)
        pl.semaphore_signal(barrier, inc=1, device_id={"bond": to}, device_id_type=MESH)
        greeted += 1
    pl.semaphore_wait(barrier, greeted)

    hops = [("row", s) for s in row_steps[:-1]] + [("bond", s) for s in bond_steps] + [("row", 1)]
    bits = [1 << (len(hops) - 1 - i) for i in range(len(hops))]
    hop_of = dict(zip(bits, hops))

    def whose(mask):
        at = {"row": me, "bond": bond}
        for bit in bits:
            if mask & bit:
                axis, s = hop_of[bit]
                at[axis] = partner(at[axis], s)
        return at["bond"] * n + at["row"]

    def omega_slot(mask):
        return omega_all.at[pl.ds(pl.multiple_of(whose(mask) * drawn, drawn), drawn), :]

    def omega_copy(mask, bit):
        axis, s = hop_of[bit]
        to = partner(me if axis == "row" else bond, s)
        return pltpu.make_async_remote_copy(
            src_ref=omega_slot(mask) if mask else omega_ref,
            dst_ref=omega_slot(mask),
            send_sem=omega_send.at[mask + bit],
            recv_sem=omega_recv.at[mask + bit],
            device_id={axis: to},
            device_id_type=MESH,
        )

    def lower_bits(mask):
        return [bit for bit in bits if mask == 0 or bit < (mask & -mask)]

    omega_order = [m for bit in bits for m in range(bit, 2 * bits[0], 2 * bit)]

    def b_copy(mask, s, k):
        at = me
        for step in row_steps:
            if mask & step:
                at = partner(at, step)
        start = pl.multiple_of(at * depth + k * piece, piece)
        target = b_all.at[pl.ds(start, piece), :]
        return pltpu.make_async_remote_copy(
            src_ref=target if mask else b_ref.at[k * piece:(k + 1) * piece, :],
            dst_ref=target,
            send_sem=b_send.at[mask + s, k],
            recv_sem=b_recv.at[mask + s, k],
            device_id={"row": partner(me, s)},
            device_id_type=MESH,
        )

    def b_lower(mask):
        return [s for s in row_steps if mask == 0 or s < (mask & -mask)]

    b_order = [m for s in row_steps for m in range(s, n, 2 * s)]

    def a_copy(j, q):
        return pltpu.make_async_remote_copy(
            src_ref=a_ref.at[pl.ds(pl.multiple_of(q * part_rows, part_rows), part_rows), :],
            dst_ref=a_all.at[slot, q],
            send_sem=a_send.at[j, q],
            recv_sem=a_recv.at[j, q],
            device_id={"row": peer(j)},
            device_id_type=MESH,
        )

    def a_arrival(j, q):
        return pltpu.make_async_remote_copy(
            src_ref=a_ref.at[pl.ds(pl.multiple_of(q * part_rows, part_rows), part_rows), :],
            dst_ref=a_all.at[lax.rem(slot + slots - j, slots), q],
            send_sem=a_send.at[j, q],
            recv_sem=a_recv.at[j, q],
            device_id={"row": peer(j)},
            device_id_type=MESH,
        )

    for bit in bits:
        omega_copy(0, bit).start()
    for s in row_steps:
        for k in range(CHUNKS):
            b_copy(0, s, k).start()
    for j in range(1, slots):
        for q in range(PARTS):
            a_copy(j, q).start()

    for q in range(PARTS):
        a_all[slot, q] = a_ref[q * part_rows:(q + 1) * part_rows, :]
    b_all[pl.ds(pl.multiple_of(me * depth, depth), depth), :] = b_ref[...]
    omega_all[pl.ds(pl.multiple_of((bond * n + me) * drawn, drawn), drawn), :] = omega_ref[...]

    def clear(i, carry):
        at = pl.ds(pl.multiple_of(i * LANES, LANES), LANES)
        high_all[at, :] = jnp.zeros((LANES, rank), BF16)
        low_all[at, :] = jnp.zeros((LANES, rank), BF16)
        gram_own[at, :] = jnp.zeros((LANES, rank), F32)
        return carry

    lax.fori_loop(0, blocks, clear, 0)

    todo = [(m, k) for m in b_order for k in range(CHUNKS)]
    every = -(-len(omega_order) // len(todo))
    steps = []
    for i, (m, k) in enumerate(todo):
        steps += [("o", o) for o in omega_order[i * every:(i + 1) * every]]
        steps.append(("b", (m, k)))
    for kind, what in steps:
        if kind == "o":
            low = what & -what
            omega_copy(what - low, low).wait_recv()
            for bit in lower_bits(what):
                omega_copy(what, bit).start()
        else:
            m, k = what
            b_copy(m - (m & -m), m & -m, k).wait_recv()
            for s in b_lower(m):
                b_copy(m, s, k).start()

    def mix(index, carry):
        j, q = lax.div(index, PARTS), lax.rem(index, PARTS)
        at = lax.rem(slot + slots - j, slots)

        @pl.when(j > 0)
        def _():
            a_arrival(j, q).wait_recv()

        base = pl.multiple_of((at * PARTS + q) * part_rows, part_rows)
        rows = pl.ds(base, part_rows)
        side = part_rows // 2
        a_turned[...] = dot(by_spin(part_rows), a_all[at, q]).astype(BF16)

        def columns(cb, carry):
            c0 = pl.multiple_of(cb * TILE, TILE)
            c1 = pl.multiple_of(bond_dim + cb * TILE, TILE)
            product = [dot(a_turned[...], b_all[:, pl.ds(c, TILE)]) for c in (c0, c1)]
            for s in range(2):
                for t in range(2):
                    total = None
                    for u in range(2):
                        for v in range(2):
                            term = gate_ref[2 * s + t, 2 * u + v] * product[v][u * side:(u + 1) * side, :]
                            total = term if total is None else total + term
                    theta[pl.ds(pl.multiple_of(base + s * side, side), side), pl.ds((c0, c1)[t], TILE)] = total.astype(BF16)
            return carry

        lax.fori_loop(0, bond_dim // TILE, columns, 0)

        def sketch(rb, carry):
            at_rank = pl.ds(pl.multiple_of(rb * TILE, TILE), TILE)
            value = dot(theta[rows, :], omega_all[:, at_rank].astype(BF16))
            w_row[rows, at_rank] = value.astype(BF16)
            w_tall[at_rank, rows] = value.T.astype(BF16)
            return carry

        lax.fori_loop(0, rank // TILE, sketch, 0)
        for i in range(rank // TILE):
            mine = slice(i * TILE, (i + 1) * TILE)
            gram_own[mine, i * TILE:] += dot(w_tall[mine, rows], w_row[rows, i * TILE:])
        return carry

    lax.fori_loop(0, slots * PARTS, mix, 0)

    def gram_copy(i):
        at = pl.ds(pl.multiple_of(i * LANES, LANES), LANES)
        return pltpu.make_async_remote_copy(
            src_ref=gram_own.at[at, :],
            dst_ref=gram_in.at[at, :],
            send_sem=gram_send.at[i],
            recv_sem=gram_recv.at[i],
            device_id={"row": near},
            device_id_type=MESH,
        )

    trace_copy = pltpu.make_async_remote_copy(
        src_ref=trace_own,
        dst_ref=trace_in,
        send_sem=trace_send,
        recv_sem=trace_recv,
        device_id={"row": near},
        device_id_type=MESH,
    )
    for i in range(blocks):
        gram_copy(i).start()
    eye = (
        lax.broadcasted_iota(jnp.int32, (LANES, LANES), 0)
        == lax.broadcasted_iota(jnp.int32, (LANES, LANES), 1)
    )
    total = jnp.zeros((LANES, LANES), F32)
    for d in range(blocks):
        at = slice(d * LANES, (d + 1) * LANES)
        total = total + jnp.where(eye, gram_own[at, at], 0.0)
    trace_own[...] = jnp.broadcast_to(jnp.sum(total, keepdims=True), (SUB, LANES))
    trace_copy.start()
    scale = 1.0 / (2.0 * bond_dim)
    trace_copy.wait()
    ridge = (trace_own[0:1, 0:1] + trace_in[0:1, 0:1]) * (scale * 0.01 / rank)

    def ahead_at(d, who):
        return ahead.at[d, :, pl.ds(pl.multiple_of(who * half, half), half), :]

    def shift_copy(d):
        return pltpu.make_async_remote_copy(
            src_ref=left_ref.at[d],
            dst_ref=ahead_at(d, me),
            send_sem=shift_send.at[d],
            recv_sem=shift_recv.at[d],
            device_id={"bond": lax.max(bond - 1, 0)},
            device_id_type=MESH,
        )

    def far_copy(j, d):
        return pltpu.make_async_remote_copy(
            src_ref=ahead_at(d, me),
            dst_ref=ahead_at(d, me),
            send_sem=far_send.at[j, d],
            recv_sem=far_recv.at[j, d],
            device_id={"row": peer(j)},
            device_id_type=MESH,
        )

    def far_arrival(j, d):
        return pltpu.make_async_remote_copy(
            src_ref=ahead_at(d, me),
            dst_ref=ahead_at(d, source(j, parity)),
            send_sem=far_send.at[j, d],
            recv_sem=far_recv.at[j, d],
            device_id={"row": peer(j)},
            device_id_type=MESH,
        )

    def near_copy(j, d, side):
        return pltpu.make_async_remote_copy(
            src_ref=ahead_at(d, source(j, side)),
            dst_ref=ahead_at(d, source(j, side)),
            send_sem=near_send.at[j, d],
            recv_sem=near_recv.at[j, d],
            device_id={"row": near},
            device_id_type=MESH,
        )

    def pass_on(d):
        shift_copy(d).wait_recv()
        for j in range(1, slots):
            far_copy(j, d).start()
        near_copy(0, d, parity).start()

    def pass_near(d):
        for j in range(1, slots):
            far_arrival(j, d).wait_recv()
            near_copy(j, d, parity).start()

    column = lax.broadcasted_iota(jnp.int32, (LANES, rank), 1)
    tall_row = lax.broadcasted_iota(jnp.int32, (rank, LANES), 0)
    ones = jnp.where(eye, 1.0, 0.0)

    def three(x):
        high, low = split(x)
        return jnp.concatenate([high, low, high], axis=0)

    def finish(d, deep):
        start = pl.multiple_of(d * LANES, LANES)
        here = pl.ds(start, LANES)
        rows = dot(factor[...], three(pending[...]))
        high_all[here, :], low_all[here, :] = split(rows)
        for ref in (high_all, low_all):
            ref[:deep, here] = jnp.where(tall_row[:deep] < start, jnp.zeros((deep, LANES), BF16), ref[:deep, here])
        high, low = split(jnp.where(column[:, :deep] < start + LANES, rows[:, :deep], 0.0))
        flat[here, :] = (dot(high, w_tall[:deep, :]) + dot(low, w_tall[:deep, :])).astype(BF16)
        side = part_rows // 2
        for q in range(PARTS):
            for s in range(2):
                first = pl.multiple_of(slot * block_rows + q * part_rows + s * side, side)
                left_ref[d, s, q * side:(q + 1) * side, :] = flat[here, pl.ds(first, side)].T

    def eliminate(deep, d, carry):
        start = pl.multiple_of(d * LANES, LANES)
        here = pl.ds(start, LANES)
        after = lax.min(d + 1, blocks - 1)
        there = pl.ds(pl.multiple_of(after * LANES, LANES), LANES)

        @pl.when(d + 1 < blocks)
        def _():
            gram_copy(d + 1).wait()

        inverse = inverse_factor(diagonal[...])
        finish(lax.max(d - 1, 0), deep)

        known = (
            dot(coeff[:LANES, :deep], high_all[:deep, :])
            + dot(coeff[LANES:, :deep], high_all[:deep, :])
            + dot(coeff[:LANES, :deep], low_all[:deep, :])
        )
        row = jnp.where(column >= start, (gram_own[here, :] + gram_in[here, :]) * scale, 0.0) - known
        pending[...] = row
        pending[:, here] = ones

        next_high, next_low = high_all[:deep, there], low_all[:deep, there]
        coeff[:LANES, :deep] = next_high.T
        coeff[LANES:, :deep] = next_low.T
        known = (
            dot(coeff[:LANES, :deep], next_high)
            + dot(coeff[LANES:, :deep], next_high)
            + dot(coeff[:LANES, :deep], next_low)
        )
        ahead_block = (gram_own[there, there] + gram_in[there, there]) * scale - known + ones * ridge

        high, low = split(inverse)
        thrice = jnp.concatenate([high, high, low], axis=1)
        factor[...] = thrice
        solved = dot(thrice, three(pending[:, there]))
        high, low = split(solved.T)
        coeff[:LANES, here] = high
        coeff[LANES:, here] = low
        diagonal[...] = ahead_block - dot(jnp.concatenate([high, high, low], axis=1), three(solved))

        @pl.when((bond > 0) & (d > 0))
        def _():
            shift_copy(d - 1).start()

        @pl.when((bond < last) & (d > 1))
        def _():
            pass_on(d - 2)

        @pl.when((bond < last) & (d > 2))
        def _():
            pass_near(d - 3)

        return carry

    pending[...] = jnp.zeros_like(pending)
    factor[...] = jnp.zeros_like(factor)
    coeff[...] = jnp.zeros_like(coeff)
    gram_copy(0).wait()
    diagonal[...] = (gram_own[:LANES, :LANES] + gram_in[:LANES, :LANES]) * scale + ones * ridge
    lax.fori_loop(0, blocks // 2, functools.partial(eliminate, rank // 2), 0)
    lax.fori_loop(blocks // 2, blocks, functools.partial(eliminate, rank), 0)
    finish(blocks - 1, rank)

    @pl.when(bond > 0)
    def _():
        shift_copy(blocks - 1).start()


    right_copy = pltpu.make_async_remote_copy(
        src_ref=right_out,
        dst_ref=right_in,
        send_sem=right_send,
        recv_sem=right_recv,
        device_id={"row": near},
        device_id_type=MESH,
    )

    right_scale = 1.0 / math.sqrt(2.0 * bond_dim)

    def project(who, store):
        ranks = pl.ds(pl.multiple_of(who * own_rank, own_rank), own_rank)

        def columns(cb, carry):
            at = pl.ds(pl.multiple_of(cb * TILE, TILE), TILE)
            store(at, dot(flat[ranks, :], theta[:, at]) * right_scale)
            return carry

        lax.fori_loop(0, 2 * bond_dim // TILE, columns, 0)

    def give(at, value):
        right_out[:, at] = value.astype(BF16)

    def keep(at, value):
        right_ref[:, at] = (value + right_in[:, at].astype(F32)).astype(BF16)

    project(near, give)
    right_copy.start()

    @pl.when(bond < last)
    def _():
        pass_on(blocks - 2)
        pass_near(blocks - 3)

    turn = interleave(block_rows)
    for d in range(0, blocks, 2):
        pair_of = [jnp.concatenate([left_ref[d + i, 0], left_ref[d + i, 1]], axis=0) for i in range(2)]
        left_out[:, d * LANES:(d + 2) * LANES] = dot(turn, jnp.concatenate(pair_of, axis=1)).astype(BF16)

    right_copy.wait()
    project(me, keep)

    @pl.when(bond < last)
    def _():
        pass_on(blocks - 1)
        pass_near(blocks - 2)


    @pl.when(bond < last)
    def _():
        stacked = jnp.concatenate([right_ref[:, :bond_dim], right_ref[:, bond_dim:]], axis=0)
        right_view[...] = dot(interleave(2 * own_rank), stacked).astype(BF16)
        odd_scale = 1.0 / math.sqrt(1.0 * bond_dim)

        def pair(d):
            for j in range(slots):
                near_copy(j, d, 1 - parity).wait_recv()
            both = jnp.concatenate([ahead[d, 0], ahead[d, 1]], axis=1)
            value = (dot(right_view[...], both) * odd_scale).astype(BF16)
            odd_ref[:, pl.ds(pl.multiple_of(d * LANES, LANES), LANES)] = value[:, :LANES]
            odd_ref[:, pl.ds(pl.multiple_of(rank + d * LANES, LANES), LANES)] = value[:, LANES:]

        def pairs(d, carry):
            pair(d)
            return carry

        lax.fori_loop(0, blocks - 1, pairs, 0)
        pass_near(blocks - 1)
        pair(blocks - 1)

        def sent(d, carry):
            for j in range(1, slots):
                far_copy(j, d).wait_send()
            for j in range(slots):
                near_copy(j, d, parity).wait_send()
            return carry

        lax.fori_loop(0, blocks, sent, 0)

    @pl.when(bond == last)
    def _():
        odd_ref[...] = jnp.zeros_like(odd_ref)

    @pl.when(bond > 0)
    def _():
        def sent(d, carry):
            shift_copy(d).wait_send()
            return carry

        lax.fori_loop(0, blocks, sent, 0)

    for mask in [0] + omega_order:
        for bit in lower_bits(mask):
            omega_copy(mask, bit).wait_send()
    for mask in [0] + b_order:
        for s in b_lower(mask):
            for k in range(CHUNKS):
                b_copy(mask, s, k).wait_send()
    for j in range(1, slots):
        for q in range(PARTS):
            a_copy(j, q).wait_send()


def layer(gate, left_site, right_site, omega, n, bonds):
    block_rows, bond_dim = left_site.shape
    part_rows = block_rows // PARTS
    depth = right_site.shape[0]
    drawn, rank = omega.shape
    slots = n // 2
    rows = slots * block_rows
    half = block_rows // 2
    own_rank = rank // n
    blocks = rank // LANES
    dma = pltpu.SemaphoreType.DMA
    return pl.pallas_call(
        functools.partial(layer_kernel, n, bonds),
        out_shape=(
            jax.ShapeDtypeStruct((block_rows, rank), BF16),
            jax.ShapeDtypeStruct((own_rank, 2 * bond_dim), BF16),
            jax.ShapeDtypeStruct((2 * own_rank, 2 * rank), BF16),
        ),
        in_specs=[pl.BlockSpec(memory_space=pltpu.SMEM)] + [pl.BlockSpec(memory_space=pltpu.VMEM)] * 3,
        out_specs=(pl.BlockSpec(memory_space=pltpu.VMEM),) * 3,
        scratch_shapes=[
            pltpu.VMEM((slots, PARTS, part_rows, bond_dim), BF16),
            pltpu.VMEM((part_rows, bond_dim), BF16),
            pltpu.VMEM((n * depth, 2 * bond_dim), BF16),
            pltpu.VMEM((bonds * n * drawn, rank), omega.dtype),
            pltpu.VMEM((rows, 2 * bond_dim), BF16),
            pltpu.VMEM((rows, rank), BF16),
            pltpu.VMEM((rank, rows), BF16),
            pltpu.VMEM((rank, rank), BF16),
            pltpu.VMEM((rank, rank), BF16),
            pltpu.VMEM((rank, rank), F32),
            pltpu.VMEM((rank, rank), F32),
            pltpu.VMEM((LANES, LANES), F32),
            pltpu.VMEM((LANES, rank), F32),
            pltpu.VMEM((LANES, 3 * LANES), BF16),
            pltpu.VMEM((2 * LANES, rank), BF16),
            pltpu.VMEM((rank, rows), BF16),
            pltpu.VMEM((blocks, 2, half, LANES), BF16),
            pltpu.VMEM((blocks, 2, n * half, LANES), BF16),
            pltpu.VMEM((own_rank, 2 * bond_dim), BF16),
            pltpu.VMEM((own_rank, 2 * bond_dim), BF16),
            pltpu.VMEM((2 * own_rank, bond_dim), BF16),
            pltpu.VMEM((SUB, LANES), F32),
            pltpu.VMEM((SUB, LANES), F32),
            dma((bonds * n,)), dma((bonds * n,)),
            dma((n, CHUNKS)), dma((n, CHUNKS)),
            dma((slots, PARTS)), dma((slots, PARTS)),
            dma((blocks,)), dma((blocks,)),
            dma, dma,
            dma((blocks,)), dma((blocks,)),
            dma((slots, blocks)), dma((slots, blocks)),
            dma((slots, blocks)), dma((slots, blocks)),
            dma, dma,
        ],
        compiler_params=pltpu.CompilerParams(
            collective_id=0, has_side_effects=True, vmem_limit_bytes=(49 if omega.dtype == BF16 else 61) * 1024 * 1024
        ),
        name="layer",
    )(gate, left_site, right_site, omega)


def shards(left_site, right_site, gate, omega):
    n, bonds = lax.axis_size("row"), lax.axis_size("bond")
    if omega.shape[0] % 16:
        omega = omega.astype(F32)
    return layer(gate, left_site, right_site, omega, n, bonds)


def solution(mesh):
    split_rows = P(("bond", "row"), None)
    return jax.shard_map(
        shards,
        mesh=mesh,
        in_specs=(split_rows, split_rows, P(), split_rows),
        out_specs=(split_rows, split_rows, split_rows),
        check_vma=False,
    )
```

```python
import functools
import math

import jax
import jax.numpy as jnp
from jax import lax
from jax.experimental import pallas as pl
from jax.experimental.pallas import tpu as pltpu
from jax.sharding import PartitionSpec as P

LANES = 128
SUB = 8
TILE = 256
PARTS = 2
CHUNKS = 8
MESH = pl.DeviceIdType.MESH
F32 = jnp.float32
BF16 = jnp.bfloat16


def partner(me, distance):
    span = 2 * distance
    return lax.div(me, span) * span + lax.rem(lax.rem(me, span) + distance, span)


def distances(n):
    found = []
    while n > 1:
        n //= 2
        found.append(n)
    return found


def split(x):
    high = x.astype(BF16)
    return high, (x - high.astype(F32)).astype(BF16)


def dot(a, b):
    return jnp.dot(a, b, preferred_element_type=F32)


def inverse_factor(block):
    groups = LANES // SUB
    lane = lax.broadcasted_iota(jnp.int32, (SUB, LANES), 1)
    sub = lax.broadcasted_iota(jnp.int32, (SUB, LANES), 0)
    rows = [block[g * SUB:(g + 1) * SUB, :] for g in range(groups)]
    finished = []

    def over_lanes(x, column):
        return jnp.broadcast_to(x[:, column:column + 1], (SUB, LANES))

    def over_rows(x, row):
        return jnp.broadcast_to(x[row:row + 1, :], (SUB, LANES))

    def inside(g):
        return (lane >= g * SUB) & (lane < (g + 1) * SUB)

    def columns(x, g):
        return [over_lanes(x, g * SUB + c) for c in range(SUB)]

    def pivots(g, cols, low=None, after=None):
        x = jnp.where(inside(g), jnp.where(lane == sub + g * SUB, 1.0, 0.0), rows[g])
        out = jnp.zeros_like(x)
        for k in range(SUB):
            here = sub == k
            root = lax.rsqrt(over_rows(cols[k], k))
            inverse = root * root
            row = over_rows(x, k)
            out = jnp.where(here, row * root, out)
            ratio = cols[k] * inverse
            x = jnp.where(here, row * inverse, x - ratio * row)
            tops = {c: over_rows(cols[c], k) for c in range(k + 1, SUB)}
            for c in range(k + 1, SUB):
                cols[c] = jnp.where(here, tops[c] * inverse, cols[c] - ratio * tops[c])
            if low is not None:
                below = low[k] * inverse
                for c in range(SUB):
                    after[c] = after[c] - below * over_rows(low[k], c)
                for c in range(k + 1, SUB):
                    low[c] = low[c] - below * tops[c]
        finished.append(jnp.where(lane <= sub + g * SUB, out, 0.0))
        return [over_rows(x, k) for k in range(SUB)]

    def remove(i, g, coeff, wide):
        rest = jnp.where(inside(g), 0.0, rows[i])
        for c in range(SUB):
            rest = rest - coeff[c] * wide[c]
        rows[i] = rest

    for g in range(0, groups, 2):
        cols = columns(rows[g], g)
        low, after = columns(rows[g + 1], g), columns(rows[g + 1], g + 1)
        wide = pivots(g, cols, list(low), after)
        remove(g + 1, g, low, wide)
        for i in range(g + 2, groups):
            remove(i, g, columns(rows[i], g), wide)
        wide = pivots(g + 1, after)
        for i in range(g + 2, groups):
            remove(i, g + 1, columns(rows[i], g + 1), wide)
    return jnp.concatenate(finished, axis=0)


def by_spin(rows):
    row = lax.broadcasted_iota(jnp.int32, (rows, rows), 0)
    col = lax.broadcasted_iota(jnp.int32, (rows, rows), 1)
    side = rows // 2
    return jnp.where(col == 2 * lax.rem(row, side) + lax.div(row, side), 1.0, 0.0).astype(BF16)


def interleave(rows):
    row = lax.broadcasted_iota(jnp.int32, (rows, rows), 0)
    col = lax.broadcasted_iota(jnp.int32, (rows, rows), 1)
    side = rows // 2
    return jnp.where(col == lax.div(row, 2) + lax.rem(row, 2) * side, 1.0, 0.0).astype(BF16)


def layer_kernel(
    n, bonds, gate_ref, a_ref, b_ref, omega_ref, left_out, right_ref, odd_ref,
    a_all, a_turned, b_all, omega_all, theta, w_row, w_tall, high_all, low_all, gram_own, gram_in,
    diagonal, pending, factor, coeff, flat, left_ref, ahead, right_out, right_in, right_view, trace_own, trace_in,
    omega_send, omega_recv, b_send, b_recv, a_send, a_recv, gram_send, gram_recv, trace_send, trace_recv,
    shift_send, shift_recv, far_send, far_recv, near_send, near_recv, right_send, right_recv,
    direct_send, direct_recv,
):
    bond, me = lax.axis_index("bond"), lax.axis_index("row")
    last = bonds - 1
    slots = n // 2
    slot, parity = lax.div(me, 2), lax.rem(me, 2)
    near = partner(me, 1)
    bond_dim = a_ref.shape[1]
    rank = omega_ref.shape[1]
    block_rows = a_ref.shape[0]
    part_rows = block_rows // PARTS
    half = block_rows // 2
    own_rank = rank // n
    blocks = rank // LANES
    depth = b_ref.shape[0]
    piece = depth // CHUNKS
    drawn = omega_ref.shape[0]

    def peer(j):
        return 2 * lax.rem(slot + j, slots) + parity

    def source(j, side):
        return 2 * lax.rem(slot + slots - j, slots) + side

    row_steps, bond_steps = distances(n), distances(bonds)

    barrier = pltpu.get_barrier_semaphore()
    greeted = 0
    for j in range(1, n):
        to = lax.rem(me + j, n)
        pl.semaphore_signal(barrier, inc=1, device_id={"row": to}, device_id_type=MESH)
        greeted += 1
    for s in bond_steps:
        pl.semaphore_signal(barrier, inc=1, device_id={"bond": partner(bond, s)}, device_id_type=MESH)
        greeted += 1
    for way in (1, last):
        to = lax.rem(bond + way, bonds)
        for j in range(slots):
            pl.semaphore_signal(barrier, inc=1, device_id={"bond": to, "row": peer(j)}, device_id_type=MESH)
            greeted += 1
    pl.semaphore_wait(barrier, greeted)

    hops = [("row", s) for s in row_steps[:-1]] + [("bond", s) for s in bond_steps] + [("row", 1)]
    bits = [1 << (len(hops) - 1 - i) for i in range(len(hops))]
    hop_of = dict(zip(bits, hops))

    def whose(mask):
        at = {"row": me, "bond": bond}
        for bit in bits:
            if mask & bit:
                axis, s = hop_of[bit]
                at[axis] = partner(at[axis], s)
        return at["bond"] * n + at["row"]

    def omega_slot(mask):
        return omega_all.at[pl.ds(pl.multiple_of(whose(mask) * drawn, drawn), drawn), :]

    def omega_copy(mask, bit):
        axis, s = hop_of[bit]
        to = partner(me if axis == "row" else bond, s)
        return pltpu.make_async_remote_copy(
            src_ref=omega_slot(mask) if mask else omega_ref,
            dst_ref=omega_slot(mask),
            send_sem=omega_send.at[mask + bit],
            recv_sem=omega_recv.at[mask + bit],
            device_id={axis: to},
            device_id_type=MESH,
        )

    def lower_bits(mask):
        return [bit for bit in bits if mask == 0 or bit < (mask & -mask)]

    omega_order = [m for bit in bits for m in range(bit, 2 * bits[0], 2 * bit)]

    def b_copy(mask, s, k):
        at = me
        for step in row_steps:
            if mask & step:
                at = partner(at, step)
        start = pl.multiple_of(at * depth + k * piece, piece)
        target = b_all.at[pl.ds(start, piece), :]
        return pltpu.make_async_remote_copy(
            src_ref=target if mask else b_ref.at[k * piece:(k + 1) * piece, :],
            dst_ref=target,
            send_sem=b_send.at[mask + s, k],
            recv_sem=b_recv.at[mask + s, k],
            device_id={"row": partner(me, s)},
            device_id_type=MESH,
        )

    def b_lower(mask):
        return [s for s in row_steps if mask == 0 or s < (mask & -mask)]

    b_order = [m for s in row_steps for m in range(s, n, 2 * s)]

    def a_copy(j, q):
        return pltpu.make_async_remote_copy(
            src_ref=a_ref.at[pl.ds(pl.multiple_of(q * part_rows, part_rows), part_rows), :],
            dst_ref=a_all.at[slot, q],
            send_sem=a_send.at[j, q],
            recv_sem=a_recv.at[j, q],
            device_id={"row": peer(j)},
            device_id_type=MESH,
        )

    def a_arrival(j, q):
        return pltpu.make_async_remote_copy(
            src_ref=a_ref.at[pl.ds(pl.multiple_of(q * part_rows, part_rows), part_rows), :],
            dst_ref=a_all.at[lax.rem(slot + slots - j, slots), q],
            send_sem=a_send.at[j, q],
            recv_sem=a_recv.at[j, q],
            device_id={"row": peer(j)},
            device_id_type=MESH,
        )

    for bit in bits:
        omega_copy(0, bit).start()
    for s in row_steps:
        for k in range(CHUNKS):
            b_copy(0, s, k).start()
    for j in range(1, slots):
        for q in range(PARTS):
            a_copy(j, q).start()

    for q in range(PARTS):
        a_all[slot, q] = a_ref[q * part_rows:(q + 1) * part_rows, :]
    b_all[pl.ds(pl.multiple_of(me * depth, depth), depth), :] = b_ref[...]
    omega_all[pl.ds(pl.multiple_of((bond * n + me) * drawn, drawn), drawn), :] = omega_ref[...]

    def clear(i, carry):
        at = pl.ds(pl.multiple_of(i * LANES, LANES), LANES)
        high_all[at, :] = jnp.zeros((LANES, rank), BF16)
        low_all[at, :] = jnp.zeros((LANES, rank), BF16)
        gram_own[at, :] = jnp.zeros((LANES, rank), F32)
        return carry

    lax.fori_loop(0, blocks, clear, 0)

    todo = [(m, k) for m in b_order for k in range(CHUNKS)]
    every = -(-len(omega_order) // len(todo))
    steps = []
    for i, (m, k) in enumerate(todo):
        steps += [("o", o) for o in omega_order[i * every:(i + 1) * every]]
        steps.append(("b", (m, k)))
    for kind, what in steps:
        if kind == "o":
            low = what & -what
            omega_copy(what - low, low).wait_recv()
            for bit in lower_bits(what):
                omega_copy(what, bit).start()
        else:
            m, k = what
            b_copy(m - (m & -m), m & -m, k).wait_recv()
            for s in b_lower(m):
                b_copy(m, s, k).start()

    def mix(index, carry):
        j, q = lax.div(index, PARTS), lax.rem(index, PARTS)
        at = lax.rem(slot + slots - j, slots)

        @pl.when(j > 0)
        def _():
            a_arrival(j, q).wait_recv()

        base = pl.multiple_of((at * PARTS + q) * part_rows, part_rows)
        rows = pl.ds(base, part_rows)
        side = part_rows // 2
        a_turned[...] = dot(by_spin(part_rows), a_all[at, q]).astype(BF16)

        def columns(cb, carry):
            c0 = pl.multiple_of(cb * TILE, TILE)
            c1 = pl.multiple_of(bond_dim + cb * TILE, TILE)
            product = [dot(a_turned[...], b_all[:, pl.ds(c, TILE)]) for c in (c0, c1)]
            for s in range(2):
                for t in range(2):
                    total = None
                    for u in range(2):
                        for v in range(2):
                            term = gate_ref[2 * s + t, 2 * u + v] * product[v][u * side:(u + 1) * side, :]
                            total = term if total is None else total + term
                    theta[pl.ds(pl.multiple_of(base + s * side, side), side), pl.ds((c0, c1)[t], TILE)] = total.astype(BF16)
            return carry

        lax.fori_loop(0, bond_dim // TILE, columns, 0)

        def sketch(rb, carry):
            at_rank = pl.ds(pl.multiple_of(rb * TILE, TILE), TILE)
            value = dot(theta[rows, :], omega_all[:, at_rank].astype(BF16))
            w_row[rows, at_rank] = value.astype(BF16)
            w_tall[at_rank, rows] = value.T.astype(BF16)
            return carry

        lax.fori_loop(0, rank // TILE, sketch, 0)
        for i in range(rank // TILE):
            mine = slice(i * TILE, (i + 1) * TILE)
            gram_own[mine, i * TILE:] += dot(w_tall[mine, rows], w_row[rows, i * TILE:])
        return carry

    lax.fori_loop(0, slots * PARTS, mix, 0)

    def gram_copy(i):
        at = pl.ds(pl.multiple_of(i * LANES, LANES), LANES)
        return pltpu.make_async_remote_copy(
            src_ref=gram_own.at[at, :],
            dst_ref=gram_in.at[at, :],
            send_sem=gram_send.at[i],
            recv_sem=gram_recv.at[i],
            device_id={"row": near},
            device_id_type=MESH,
        )

    trace_copy = pltpu.make_async_remote_copy(
        src_ref=trace_own,
        dst_ref=trace_in,
        send_sem=trace_send,
        recv_sem=trace_recv,
        device_id={"row": near},
        device_id_type=MESH,
    )
    eye = (
        lax.broadcasted_iota(jnp.int32, (LANES, LANES), 0)
        == lax.broadcasted_iota(jnp.int32, (LANES, LANES), 1)
    )
    total = jnp.zeros((LANES, LANES), F32)
    for d in range(blocks):
        at = slice(d * LANES, (d + 1) * LANES)
        total = total + jnp.where(eye, gram_own[at, at], 0.0)
    trace_own[...] = jnp.broadcast_to(jnp.sum(total, keepdims=True), (SUB, LANES))
    trace_copy.start()
    for i in range(blocks):
        gram_copy(i).start()
    scale = 1.0 / (2.0 * bond_dim)
    trace_copy.wait()
    ridge = (trace_own[0:1, 0:1] + trace_in[0:1, 0:1]) * (scale * 0.01 / rank)

    def ahead_at(d, who):
        return ahead.at[d, :, pl.ds(pl.multiple_of(who * half, half), half), :]

    def shift_copy(d):
        return pltpu.make_async_remote_copy(
            src_ref=left_ref.at[d],
            dst_ref=ahead_at(d, me),
            send_sem=shift_send.at[d],
            recv_sem=shift_recv.at[d],
            device_id={"bond": lax.max(bond - 1, 0)},
            device_id_type=MESH,
        )

    def far_copy(j, d):
        return pltpu.make_async_remote_copy(
            src_ref=ahead_at(d, me),
            dst_ref=ahead_at(d, me),
            send_sem=far_send.at[j, d],
            recv_sem=far_recv.at[j, d],
            device_id={"row": peer(j)},
            device_id_type=MESH,
        )

    def far_arrival(j, d):
        return pltpu.make_async_remote_copy(
            src_ref=ahead_at(d, me),
            dst_ref=ahead_at(d, source(j, parity)),
            send_sem=far_send.at[j, d],
            recv_sem=far_recv.at[j, d],
            device_id={"row": peer(j)},
            device_id_type=MESH,
        )

    def near_copy(j, d, side):
        return pltpu.make_async_remote_copy(
            src_ref=ahead_at(d, source(j, side)),
            dst_ref=ahead_at(d, source(j, side)),
            send_sem=near_send.at[j, d],
            recv_sem=near_recv.at[j, d],
            device_id={"row": near},
            device_id_type=MESH,
        )

    def direct_copy(j):
        return pltpu.make_async_remote_copy(
            src_ref=left_ref.at[blocks - 1],
            dst_ref=ahead_at(blocks - 1, me),
            send_sem=direct_send.at[j],
            recv_sem=direct_recv.at[j],
            device_id={"bond": lax.max(bond - 1, 0), "row": peer(j)},
            device_id_type=MESH,
        )

    def direct_arrival(j):
        return pltpu.make_async_remote_copy(
            src_ref=left_ref.at[blocks - 1],
            dst_ref=ahead_at(blocks - 1, source(j, parity)),
            send_sem=direct_send.at[j],
            recv_sem=direct_recv.at[j],
            device_id={"bond": lax.max(bond - 1, 0), "row": peer(j)},
            device_id_type=MESH,
        )

    def pass_on(d):
        shift_copy(d).wait_recv()
        for j in range(1, slots):
            far_copy(j, d).start()
        near_copy(0, d, parity).start()

    def pass_near(d):
        for j in range(1, slots):
            far_arrival(j, d).wait_recv()
            near_copy(j, d, parity).start()

    column = lax.broadcasted_iota(jnp.int32, (LANES, rank), 1)
    tall_row = lax.broadcasted_iota(jnp.int32, (rank, LANES), 0)
    ones = jnp.where(eye, 1.0, 0.0)

    def three(x):
        high, low = split(x)
        return jnp.concatenate([high, low, high], axis=0)

    def finish(d, deep):
        start = pl.multiple_of(d * LANES, LANES)
        here = pl.ds(start, LANES)
        rows = dot(factor[...], three(pending[...]))
        high_all[here, :], low_all[here, :] = split(rows)
        for ref in (high_all, low_all):
            ref[:deep, here] = jnp.where(tall_row[:deep] < start, jnp.zeros((deep, LANES), BF16), ref[:deep, here])
        high, low = split(jnp.where(column[:, :deep] < start + LANES, rows[:, :deep], 0.0))
        own = pl.ds(pl.multiple_of(slot * block_rows, block_rows), block_rows)
        flat[here, own] = (dot(high, w_tall[:deep, own]) + dot(low, w_tall[:deep, own])).astype(BF16)
        side = part_rows // 2
        for q in range(PARTS):
            for s in range(2):
                first = pl.multiple_of(slot * block_rows + q * part_rows + s * side, side)
                left_ref[d, s, q * side:(q + 1) * side, :] = flat[here, pl.ds(first, side)].T

    def eliminate(deep, d, carry):
        start = pl.multiple_of(d * LANES, LANES)
        here = pl.ds(start, LANES)
        after = lax.min(d + 1, blocks - 1)
        there = pl.ds(pl.multiple_of(after * LANES, LANES), LANES)

        @pl.when(d + 1 < blocks)
        def _():
            gram_copy(d + 1).wait()

        inverse = inverse_factor(diagonal[...])
        finish(lax.max(d - 1, 0), deep)

        known = (
            dot(coeff[:LANES, :deep], high_all[:deep, :])
            + dot(coeff[LANES:, :deep], high_all[:deep, :])
            + dot(coeff[:LANES, :deep], low_all[:deep, :])
        )
        row = jnp.where(column >= start, (gram_own[here, :] + gram_in[here, :]) * scale, 0.0) - known
        pending[...] = row
        pending[:, here] = ones

        next_high, next_low = high_all[:deep, there], low_all[:deep, there]
        coeff[:LANES, :deep] = next_high.T
        coeff[LANES:, :deep] = next_low.T
        known = (
            dot(coeff[:LANES, :deep], next_high)
            + dot(coeff[LANES:, :deep], next_high)
            + dot(coeff[:LANES, :deep], next_low)
        )
        ahead_block = (gram_own[there, there] + gram_in[there, there]) * scale - known + ones * ridge

        high, low = split(inverse)
        thrice = jnp.concatenate([high, high, low], axis=1)
        factor[...] = thrice
        solved = dot(thrice, three(pending[:, there]))
        high, low = split(solved.T)
        coeff[:LANES, here] = high
        coeff[LANES:, here] = low
        diagonal[...] = ahead_block - dot(jnp.concatenate([high, high, low], axis=1), three(solved))

        @pl.when((bond > 0) & (d > 0))
        def _():
            shift_copy(d - 1).start()

        @pl.when((bond < last) & (d > 1))
        def _():
            pass_on(d - 2)

        @pl.when((bond < last) & (d > 2))
        def _():
            pass_near(d - 3)

        return carry

    pending[...] = jnp.zeros_like(pending)
    factor[...] = jnp.zeros_like(factor)
    coeff[...] = jnp.zeros_like(coeff)
    gram_copy(0).wait()
    diagonal[...] = (gram_own[:LANES, :LANES] + gram_in[:LANES, :LANES]) * scale + ones * ridge
    lax.fori_loop(0, blocks // 2, functools.partial(eliminate, rank // 2), 0)
    lax.fori_loop(blocks // 2, blocks, functools.partial(eliminate, rank), 0)
    finish(blocks - 1, rank)

    @pl.when(bond > 0)
    def _():
        shift_copy(blocks - 1).start()
        for j in range(1, slots):
            direct_copy(j).start()


    right_copy = pltpu.make_async_remote_copy(
        src_ref=right_out,
        dst_ref=right_in,
        send_sem=right_send,
        recv_sem=right_recv,
        device_id={"row": near},
        device_id_type=MESH,
    )

    right_scale = 1.0 / math.sqrt(2.0 * bond_dim)

    def project(who, store):
        ranks = pl.ds(pl.multiple_of(who * own_rank, own_rank), own_rank)

        def columns(cb, carry):
            at = pl.ds(pl.multiple_of(cb * TILE, TILE), TILE)
            store(at, dot(flat[ranks, :], theta[:, at]) * right_scale)
            return carry

        lax.fori_loop(0, 2 * bond_dim // TILE, columns, 0)

    def give(at, value):
        right_out[:, at] = value.astype(BF16)

    def keep(at, value):
        right_ref[:, at] = (value + right_in[:, at].astype(F32)).astype(BF16)

    pair_ranks = pl.ds(pl.multiple_of(slot * 2 * own_rank, 2 * own_rank), 2 * own_rank)
    for j in range(1, slots):
        at = pl.ds(pl.multiple_of(lax.rem(slot + j, slots) * block_rows, block_rows), block_rows)
        flat[pair_ranks, at] = (
            dot(high_all[pair_ranks, :], w_tall[:, at]) + dot(low_all[pair_ranks, :], w_tall[:, at])
        ).astype(BF16)

    project(near, give)
    right_copy.start()

    @pl.when(bond < last)
    def _():
        pass_on(blocks - 2)
        pass_near(blocks - 3)

    turn = interleave(block_rows)
    for d in range(0, blocks, 2):
        pair_of = [jnp.concatenate([left_ref[d + i, 0], left_ref[d + i, 1]], axis=0) for i in range(2)]
        left_out[:, d * LANES:(d + 2) * LANES] = dot(turn, jnp.concatenate(pair_of, axis=1)).astype(BF16)

    right_copy.wait()
    project(me, keep)

    @pl.when(bond < last)
    def _():
        pass_near(blocks - 2)
        shift_copy(blocks - 1).wait_recv()
        near_copy(0, blocks - 1, parity).start()

    @pl.when(bond < last)
    def _():
        stacked = jnp.concatenate([right_ref[:, :bond_dim], right_ref[:, bond_dim:]], axis=0)
        right_view[...] = dot(interleave(2 * own_rank), stacked).astype(BF16)
        odd_scale = 1.0 / math.sqrt(1.0 * bond_dim)

        def pair(d):
            for j in range(slots):
                near_copy(j, d, 1 - parity).wait_recv()
            both = jnp.concatenate([ahead[d, 0], ahead[d, 1]], axis=1)
            value = (dot(right_view[...], both) * odd_scale).astype(BF16)
            odd_ref[:, pl.ds(pl.multiple_of(d * LANES, LANES), LANES)] = value[:, :LANES]
            odd_ref[:, pl.ds(pl.multiple_of(rank + d * LANES, LANES), LANES)] = value[:, LANES:]

        def pairs(d, carry):
            pair(d)
            return carry

        lax.fori_loop(0, blocks - 1, pairs, 0)
        for j in range(1, slots):
            direct_arrival(j).wait_recv()
            near_copy(j, blocks - 1, parity).start()
        pair(blocks - 1)

        def sent(d, carry):
            for j in range(slots):
                near_copy(j, d, parity).wait_send()
            return carry

        def sent_far(d, carry):
            for j in range(1, slots):
                far_copy(j, d).wait_send()
            return carry

        lax.fori_loop(0, blocks - 1, sent_far, 0)

        lax.fori_loop(0, blocks, sent, 0)

    @pl.when(bond == last)
    def _():
        odd_ref[...] = jnp.zeros_like(odd_ref)

    @pl.when(bond > 0)
    def _():
        def sent(d, carry):
            shift_copy(d).wait_send()
            return carry

        lax.fori_loop(0, blocks, sent, 0)
        for j in range(1, slots):
            direct_copy(j).wait_send()

    for mask in [0] + omega_order:
        for bit in lower_bits(mask):
            omega_copy(mask, bit).wait_send()
    for mask in [0] + b_order:
        for s in b_lower(mask):
            for k in range(CHUNKS):
                b_copy(mask, s, k).wait_send()
    for j in range(1, slots):
        for q in range(PARTS):
            a_copy(j, q).wait_send()


def layer(gate, left_site, right_site, omega, n, bonds):
    block_rows, bond_dim = left_site.shape
    part_rows = block_rows // PARTS
    depth = right_site.shape[0]
    drawn, rank = omega.shape
    slots = n // 2
    rows = slots * block_rows
    half = block_rows // 2
    own_rank = rank // n
    blocks = rank // LANES
    dma = pltpu.SemaphoreType.DMA
    return pl.pallas_call(
        functools.partial(layer_kernel, n, bonds),
        out_shape=(
            jax.ShapeDtypeStruct((block_rows, rank), BF16),
            jax.ShapeDtypeStruct((own_rank, 2 * bond_dim), BF16),
            jax.ShapeDtypeStruct((2 * own_rank, 2 * rank), BF16),
        ),
        in_specs=[pl.BlockSpec(memory_space=pltpu.SMEM)] + [pl.BlockSpec(memory_space=pltpu.VMEM)] * 3,
        out_specs=(pl.BlockSpec(memory_space=pltpu.VMEM),) * 3,
        scratch_shapes=[
            pltpu.VMEM((slots, PARTS, part_rows, bond_dim), BF16),
            pltpu.VMEM((part_rows, bond_dim), BF16),
            pltpu.VMEM((n * depth, 2 * bond_dim), BF16),
            pltpu.VMEM((bonds * n * drawn, rank), omega.dtype),
            pltpu.VMEM((rows, 2 * bond_dim), BF16),
            pltpu.VMEM((rows, rank), BF16),
            pltpu.VMEM((rank, rows), BF16),
            pltpu.VMEM((rank, rank), BF16),
            pltpu.VMEM((rank, rank), BF16),
            pltpu.VMEM((rank, rank), F32),
            pltpu.VMEM((rank, rank), F32),
            pltpu.VMEM((LANES, LANES), F32),
            pltpu.VMEM((LANES, rank), F32),
            pltpu.VMEM((LANES, 3 * LANES), BF16),
            pltpu.VMEM((2 * LANES, rank), BF16),
            pltpu.VMEM((rank, rows), BF16),
            pltpu.VMEM((blocks, 2, half, LANES), BF16),
            pltpu.VMEM((blocks, 2, n * half, LANES), BF16),
            pltpu.VMEM((own_rank, 2 * bond_dim), BF16),
            pltpu.VMEM((own_rank, 2 * bond_dim), BF16),
            pltpu.VMEM((2 * own_rank, bond_dim), BF16),
            pltpu.VMEM((SUB, LANES), F32),
            pltpu.VMEM((SUB, LANES), F32),
            dma((bonds * n,)), dma((bonds * n,)),
            dma((n, CHUNKS)), dma((n, CHUNKS)),
            dma((slots, PARTS)), dma((slots, PARTS)),
            dma((blocks,)), dma((blocks,)),
            dma, dma,
            dma((blocks,)), dma((blocks,)),
            dma((slots, blocks)), dma((slots, blocks)),
            dma((slots, blocks)), dma((slots, blocks)),
            dma, dma,
            dma((slots,)), dma((slots,)),
        ],
        compiler_params=pltpu.CompilerParams(
            collective_id=0, has_side_effects=True, vmem_limit_bytes=(49 if omega.dtype == BF16 else 61) * 1024 * 1024
        ),
        name="layer",
    )(gate, left_site, right_site, omega)


def shards(left_site, right_site, gate, omega):
    n, bonds = lax.axis_size("row"), lax.axis_size("bond")
    if omega.shape[0] % 16:
        omega = omega.astype(F32)
    return layer(gate, left_site, right_site, omega, n, bonds)


def solution(mesh):
    split_rows = P(("bond", "row"), None)
    return jax.shard_map(
        shards,
        mesh=mesh,
        in_specs=(split_rows, split_rows, P(), split_rows),
        out_specs=(split_rows, split_rows, split_rows),
        check_vma=False,
    )
```

```python
import functools
import math

import jax
import jax.numpy as jnp
from jax import lax
from jax.experimental import pallas as pl
from jax.experimental.pallas import tpu as pltpu
from jax.sharding import PartitionSpec as P

LANES = 128
SUB = 8
TILE = 256
PARTS = 2
CHUNKS = 8
MESH = pl.DeviceIdType.MESH
F32 = jnp.float32
BF16 = jnp.bfloat16


def partner(me, distance):
    span = 2 * distance
    return lax.div(me, span) * span + lax.rem(lax.rem(me, span) + distance, span)


def distances(n):
    found = []
    while n > 1:
        n //= 2
        found.append(n)
    return found


def split(x):
    high = x.astype(BF16)
    return high, (x - high.astype(F32)).astype(BF16)


def dot(a, b):
    return jnp.dot(a, b, preferred_element_type=F32)


def inverse_factor(block):
    groups = LANES // SUB
    lane = lax.broadcasted_iota(jnp.int32, (SUB, LANES), 1)
    sub = lax.broadcasted_iota(jnp.int32, (SUB, LANES), 0)
    rows = [block[g * SUB:(g + 1) * SUB, :] for g in range(groups)]
    finished = []

    def over_lanes(x, column):
        return jnp.broadcast_to(x[:, column:column + 1], (SUB, LANES))

    def over_rows(x, row):
        return jnp.broadcast_to(x[row:row + 1, :], (SUB, LANES))

    def inside(g):
        return (lane >= g * SUB) & (lane < (g + 1) * SUB)

    def columns(x, g):
        return [over_lanes(x, g * SUB + c) for c in range(SUB)]

    def pivots(g, cols, low=None, after=None):
        x = jnp.where(inside(g), jnp.where(lane == sub + g * SUB, 1.0, 0.0), rows[g])
        out = jnp.zeros_like(x)
        for k in range(SUB):
            here = sub == k
            root = lax.rsqrt(over_rows(cols[k], k))
            inverse = root * root
            row = over_rows(x, k)
            out = jnp.where(here, row * root, out)
            ratio = cols[k] * inverse
            x = jnp.where(here, row * inverse, x - ratio * row)
            tops = {c: over_rows(cols[c], k) for c in range(k + 1, SUB)}
            for c in range(k + 1, SUB):
                cols[c] = jnp.where(here, tops[c] * inverse, cols[c] - ratio * tops[c])
            if low is not None:
                below = low[k] * inverse
                for c in range(SUB):
                    after[c] = after[c] - below * over_rows(low[k], c)
                for c in range(k + 1, SUB):
                    low[c] = low[c] - below * tops[c]
        finished.append(jnp.where(lane <= sub + g * SUB, out, 0.0))
        return [over_rows(x, k) for k in range(SUB)]

    def remove(i, g, coeff, wide):
        rest = jnp.where(inside(g), 0.0, rows[i])
        for c in range(SUB):
            rest = rest - coeff[c] * wide[c]
        rows[i] = rest

    for g in range(0, groups, 2):
        cols = columns(rows[g], g)
        low, after = columns(rows[g + 1], g), columns(rows[g + 1], g + 1)
        wide = pivots(g, cols, list(low), after)
        remove(g + 1, g, low, wide)
        for i in range(g + 2, groups):
            remove(i, g, columns(rows[i], g), wide)
        wide = pivots(g + 1, after)
        for i in range(g + 2, groups):
            remove(i, g + 1, columns(rows[i], g + 1), wide)
    return jnp.concatenate(finished, axis=0)


def by_spin(rows):
    row = lax.broadcasted_iota(jnp.int32, (rows, rows), 0)
    col = lax.broadcasted_iota(jnp.int32, (rows, rows), 1)
    side = rows // 2
    return jnp.where(col == 2 * lax.rem(row, side) + lax.div(row, side), 1.0, 0.0).astype(BF16)


def interleave(rows):
    row = lax.broadcasted_iota(jnp.int32, (rows, rows), 0)
    col = lax.broadcasted_iota(jnp.int32, (rows, rows), 1)
    side = rows // 2
    return jnp.where(col == lax.div(row, 2) + lax.rem(row, 2) * side, 1.0, 0.0).astype(BF16)


def layer_kernel(
    n, bonds, gate_hbm, a_ref, b_ref, omega_ref, left_out, right_ref, odd_ref,
    a_all, a_turned, b_all, omega_all, theta, w_row, w_tall, high_all, low_all, gram_own, gram_in,
    diagonal, pending, factor, coeff, flat, left_ref, ahead, right_out, right_in, right_view, trace_own, trace_in,
    omega_send, omega_recv, b_send, b_recv, a_send, a_recv, gram_send, gram_recv, trace_send, trace_recv,
    shift_send, shift_recv, far_send, far_recv, near_send, near_recv, right_send, right_recv,
    direct_send, direct_recv, load_sem, gate_sem, gate_ref,
):
    bond, me = lax.axis_index("bond"), lax.axis_index("row")
    last = bonds - 1
    slots = n // 2
    slot, parity = lax.div(me, 2), lax.rem(me, 2)
    near = partner(me, 1)
    bond_dim = a_ref.shape[1]
    rank = omega_ref.shape[1]
    block_rows = a_ref.shape[0]
    part_rows = block_rows // PARTS
    half = block_rows // 2
    own_rank = rank // n
    blocks = rank // LANES
    depth = b_ref.shape[0]
    piece = depth // CHUNKS
    drawn = omega_ref.shape[0]

    def peer(j):
        return 2 * lax.rem(slot + j, slots) + parity

    def source(j, side):
        return 2 * lax.rem(slot + slots - j, slots) + side

    row_steps, bond_steps = distances(n), distances(bonds)

    own_depth = pl.ds(pl.multiple_of(me * depth, depth), depth)
    own_drawn = pl.ds(pl.multiple_of((bond * n + me) * drawn, drawn), drawn)
    loads = [
        pltpu.make_async_copy(omega_ref, omega_all.at[own_drawn, :], load_sem.at[0]),
        pltpu.make_async_copy(b_ref, b_all.at[own_depth, :], load_sem.at[1]),
    ]
    for q in range(PARTS):
        rows = pl.ds(q * part_rows, part_rows)
        loads.append(pltpu.make_async_copy(a_ref.at[rows, :], a_all.at[slot, q], load_sem.at[2 + q]))
    gate_load = pltpu.make_async_copy(gate_hbm, gate_ref, gate_sem)
    for load in loads:
        load.start()
    gate_load.start()

    barrier = pltpu.get_barrier_semaphore()
    greeted = 0
    for j in range(1, n):
        to = lax.rem(me + j, n)
        pl.semaphore_signal(barrier, inc=1, device_id={"row": to}, device_id_type=MESH)
        greeted += 1
    for s in bond_steps:
        pl.semaphore_signal(barrier, inc=1, device_id={"bond": partner(bond, s)}, device_id_type=MESH)
        greeted += 1
    for way in (1, last):
        to = lax.rem(bond + way, bonds)
        for j in range(slots):
            pl.semaphore_signal(barrier, inc=1, device_id={"bond": to, "row": peer(j)}, device_id_type=MESH)
            greeted += 1
    pl.semaphore_wait(barrier, greeted)

    hops = [("row", s) for s in row_steps[:-1]] + [("bond", s) for s in bond_steps] + [("row", 1)]
    bits = [1 << (len(hops) - 1 - i) for i in range(len(hops))]
    hop_of = dict(zip(bits, hops))

    def whose(mask):
        at = {"row": me, "bond": bond}
        for bit in bits:
            if mask & bit:
                axis, s = hop_of[bit]
                at[axis] = partner(at[axis], s)
        return at["bond"] * n + at["row"]

    def omega_slot(mask):
        return omega_all.at[pl.ds(pl.multiple_of(whose(mask) * drawn, drawn), drawn), :]

    def omega_copy(mask, bit):
        axis, s = hop_of[bit]
        to = partner(me if axis == "row" else bond, s)
        return pltpu.make_async_remote_copy(
            src_ref=omega_slot(mask),
            dst_ref=omega_slot(mask),
            send_sem=omega_send.at[mask + bit],
            recv_sem=omega_recv.at[mask + bit],
            device_id={axis: to},
            device_id_type=MESH,
        )

    def lower_bits(mask):
        return [bit for bit in bits if mask == 0 or bit < (mask & -mask)]

    omega_order = [m for bit in bits for m in range(bit, 2 * bits[0], 2 * bit)]

    def b_copy(mask, s, k):
        at = me
        for step in row_steps:
            if mask & step:
                at = partner(at, step)
        start = pl.multiple_of(at * depth + k * piece, piece)
        target = b_all.at[pl.ds(start, piece), :]
        return pltpu.make_async_remote_copy(
            src_ref=target,
            dst_ref=target,
            send_sem=b_send.at[mask + s, k],
            recv_sem=b_recv.at[mask + s, k],
            device_id={"row": partner(me, s)},
            device_id_type=MESH,
        )

    def b_lower(mask):
        return [s for s in row_steps if mask == 0 or s < (mask & -mask)]

    b_order = [m for s in row_steps for m in range(s, n, 2 * s)]

    def a_copy(j, q):
        return pltpu.make_async_remote_copy(
            src_ref=a_all.at[slot, q],
            dst_ref=a_all.at[slot, q],
            send_sem=a_send.at[j, q],
            recv_sem=a_recv.at[j, q],
            device_id={"row": peer(j)},
            device_id_type=MESH,
        )

    def a_arrival(j, q):
        return pltpu.make_async_remote_copy(
            src_ref=a_all.at[slot, q],
            dst_ref=a_all.at[lax.rem(slot + slots - j, slots), q],
            send_sem=a_send.at[j, q],
            recv_sem=a_recv.at[j, q],
            device_id={"row": peer(j)},
            device_id_type=MESH,
        )

    loads[0].wait()
    for bit in bits:
        omega_copy(0, bit).start()
    loads[1].wait()
    for s in row_steps:
        for k in range(CHUNKS):
            b_copy(0, s, k).start()
    for q in range(PARTS):
        loads[2 + q].wait()
        for j in range(1, slots):
            a_copy(j, q).start()
    gate_load.wait()

    def clear(i, carry):
        at = pl.ds(pl.multiple_of(i * LANES, LANES), LANES)
        high_all[at, :] = jnp.zeros((LANES, rank), BF16)
        low_all[at, :] = jnp.zeros((LANES, rank), BF16)
        gram_own[at, :] = jnp.zeros((LANES, rank), F32)
        return carry

    lax.fori_loop(0, blocks, clear, 0)

    todo = [(m, k) for m in b_order for k in range(CHUNKS)]
    every = -(-len(omega_order) // len(todo))
    steps = []
    for i, (m, k) in enumerate(todo):
        steps += [("o", o) for o in omega_order[i * every:(i + 1) * every]]
        steps.append(("b", (m, k)))
    for kind, what in steps:
        if kind == "o":
            low = what & -what
            omega_copy(what - low, low).wait_recv()
            for bit in lower_bits(what):
                omega_copy(what, bit).start()
        else:
            m, k = what
            b_copy(m - (m & -m), m & -m, k).wait_recv()
            for s in b_lower(m):
                b_copy(m, s, k).start()

    def mix(index, carry):
        j, q = lax.div(index, PARTS), lax.rem(index, PARTS)
        at = lax.rem(slot + slots - j, slots)

        @pl.when(j > 0)
        def _():
            a_arrival(j, q).wait_recv()

        base = pl.multiple_of((at * PARTS + q) * part_rows, part_rows)
        rows = pl.ds(base, part_rows)
        side = part_rows // 2
        a_turned[...] = dot(by_spin(part_rows), a_all[at, q]).astype(BF16)

        def columns(cb, carry):
            c0 = pl.multiple_of(cb * TILE, TILE)
            c1 = pl.multiple_of(bond_dim + cb * TILE, TILE)
            product = [dot(a_turned[...], b_all[:, pl.ds(c, TILE)]) for c in (c0, c1)]
            for s in range(2):
                for t in range(2):
                    total = None
                    for u in range(2):
                        for v in range(2):
                            term = gate_ref[2 * s + t, 2 * u + v] * product[v][u * side:(u + 1) * side, :]
                            total = term if total is None else total + term
                    theta[pl.ds(pl.multiple_of(base + s * side, side), side), pl.ds((c0, c1)[t], TILE)] = total.astype(BF16)
            return carry

        lax.fori_loop(0, bond_dim // TILE, columns, 0)

        def sketch(rb, carry):
            at_rank = pl.ds(pl.multiple_of(rb * TILE, TILE), TILE)
            value = dot(theta[rows, :], omega_all[:, at_rank].astype(BF16))
            w_row[rows, at_rank] = value.astype(BF16)
            w_tall[at_rank, rows] = value.T.astype(BF16)
            return carry

        lax.fori_loop(0, rank // TILE, sketch, 0)
        for i in range(rank // TILE):
            mine = slice(i * TILE, (i + 1) * TILE)
            gram_own[mine, i * TILE:] += dot(w_tall[mine, rows], w_row[rows, i * TILE:])
        return carry

    lax.fori_loop(0, slots * PARTS, mix, 0)

    def gram_copy(i):
        at = pl.ds(pl.multiple_of(i * LANES, LANES), LANES)
        return pltpu.make_async_remote_copy(
            src_ref=gram_own.at[at, :],
            dst_ref=gram_in.at[at, :],
            send_sem=gram_send.at[i],
            recv_sem=gram_recv.at[i],
            device_id={"row": near},
            device_id_type=MESH,
        )

    trace_copy = pltpu.make_async_remote_copy(
        src_ref=trace_own,
        dst_ref=trace_in,
        send_sem=trace_send,
        recv_sem=trace_recv,
        device_id={"row": near},
        device_id_type=MESH,
    )
    eye = (
        lax.broadcasted_iota(jnp.int32, (LANES, LANES), 0)
        == lax.broadcasted_iota(jnp.int32, (LANES, LANES), 1)
    )
    total = jnp.zeros((LANES, LANES), F32)
    for d in range(blocks):
        at = slice(d * LANES, (d + 1) * LANES)
        total = total + jnp.where(eye, gram_own[at, at], 0.0)
    trace_own[...] = jnp.broadcast_to(jnp.sum(total, keepdims=True), (SUB, LANES))
    trace_copy.start()
    for i in range(blocks):
        gram_copy(i).start()
    scale = 1.0 / (2.0 * bond_dim)
    trace_copy.wait()
    ridge = (trace_own[0:1, 0:1] + trace_in[0:1, 0:1]) * (scale * 0.01 / rank)

    def ahead_at(d, who):
        return ahead.at[d, :, pl.ds(pl.multiple_of(who * half, half), half), :]

    def shift_copy(d):
        return pltpu.make_async_remote_copy(
            src_ref=left_ref.at[d],
            dst_ref=ahead_at(d, me),
            send_sem=shift_send.at[d],
            recv_sem=shift_recv.at[d],
            device_id={"bond": lax.max(bond - 1, 0)},
            device_id_type=MESH,
        )

    def far_copy(j, d):
        return pltpu.make_async_remote_copy(
            src_ref=ahead_at(d, me),
            dst_ref=ahead_at(d, me),
            send_sem=far_send.at[j, d],
            recv_sem=far_recv.at[j, d],
            device_id={"row": peer(j)},
            device_id_type=MESH,
        )

    def far_arrival(j, d):
        return pltpu.make_async_remote_copy(
            src_ref=ahead_at(d, me),
            dst_ref=ahead_at(d, source(j, parity)),
            send_sem=far_send.at[j, d],
            recv_sem=far_recv.at[j, d],
            device_id={"row": peer(j)},
            device_id_type=MESH,
        )

    def near_copy(j, d, side):
        return pltpu.make_async_remote_copy(
            src_ref=ahead_at(d, source(j, side)),
            dst_ref=ahead_at(d, source(j, side)),
            send_sem=near_send.at[j, d],
            recv_sem=near_recv.at[j, d],
            device_id={"row": near},
            device_id_type=MESH,
        )

    def direct_copy(j):
        return pltpu.make_async_remote_copy(
            src_ref=left_ref.at[blocks - 1],
            dst_ref=ahead_at(blocks - 1, me),
            send_sem=direct_send.at[j],
            recv_sem=direct_recv.at[j],
            device_id={"bond": lax.max(bond - 1, 0), "row": peer(j)},
            device_id_type=MESH,
        )

    def direct_arrival(j):
        return pltpu.make_async_remote_copy(
            src_ref=left_ref.at[blocks - 1],
            dst_ref=ahead_at(blocks - 1, source(j, parity)),
            send_sem=direct_send.at[j],
            recv_sem=direct_recv.at[j],
            device_id={"bond": lax.max(bond - 1, 0), "row": peer(j)},
            device_id_type=MESH,
        )

    def pass_on(d):
        shift_copy(d).wait_recv()
        for j in range(1, slots):
            far_copy(j, d).start()
        near_copy(0, d, parity).start()

    def pass_near(d):
        for j in range(1, slots):
            far_arrival(j, d).wait_recv()
            near_copy(j, d, parity).start()

    column = lax.broadcasted_iota(jnp.int32, (LANES, rank), 1)
    tall_row = lax.broadcasted_iota(jnp.int32, (rank, LANES), 0)
    ones = jnp.where(eye, 1.0, 0.0)

    def three(x):
        high, low = split(x)
        return jnp.concatenate([high, low, high], axis=0)

    def finish(d, deep):
        start = pl.multiple_of(d * LANES, LANES)
        here = pl.ds(start, LANES)
        rows = dot(factor[...], three(pending[...]))
        high_all[here, :], low_all[here, :] = split(rows)
        for ref in (high_all, low_all):
            ref[:deep, here] = jnp.where(tall_row[:deep] < start, jnp.zeros((deep, LANES), BF16), ref[:deep, here])
        high, low = split(jnp.where(column[:, :deep] < start + LANES, rows[:, :deep], 0.0))
        own = pl.ds(pl.multiple_of(slot * block_rows, block_rows), block_rows)
        flat[here, own] = (dot(high, w_tall[:deep, own]) + dot(low, w_tall[:deep, own])).astype(BF16)
        side = part_rows // 2
        for q in range(PARTS):
            for s in range(2):
                first = pl.multiple_of(slot * block_rows + q * part_rows + s * side, side)
                left_ref[d, s, q * side:(q + 1) * side, :] = flat[here, pl.ds(first, side)].T

    def eliminate(deep, d, carry):
        start = pl.multiple_of(d * LANES, LANES)
        here = pl.ds(start, LANES)
        after = lax.min(d + 1, blocks - 1)
        there = pl.ds(pl.multiple_of(after * LANES, LANES), LANES)

        @pl.when(d + 1 < blocks)
        def _():
            gram_copy(d + 1).wait()

        inverse = inverse_factor(diagonal[...])
        finish(lax.max(d - 1, 0), deep)

        known = (
            dot(coeff[:LANES, :deep], high_all[:deep, :])
            + dot(coeff[LANES:, :deep], high_all[:deep, :])
            + dot(coeff[:LANES, :deep], low_all[:deep, :])
        )
        row = jnp.where(column >= start, (gram_own[here, :] + gram_in[here, :]) * scale, 0.0) - known
        pending[...] = row
        pending[:, here] = ones

        next_high, next_low = high_all[:deep, there], low_all[:deep, there]
        coeff[:LANES, :deep] = next_high.T
        coeff[LANES:, :deep] = next_low.T
        known = (
            dot(coeff[:LANES, :deep], next_high)
            + dot(coeff[LANES:, :deep], next_high)
            + dot(coeff[:LANES, :deep], next_low)
        )
        ahead_block = (gram_own[there, there] + gram_in[there, there]) * scale - known + ones * ridge

        high, low = split(inverse)
        thrice = jnp.concatenate([high, high, low], axis=1)
        factor[...] = thrice
        solved = dot(thrice, three(pending[:, there]))
        high, low = split(solved.T)
        coeff[:LANES, here] = high
        coeff[LANES:, here] = low
        diagonal[...] = ahead_block - dot(jnp.concatenate([high, high, low], axis=1), three(solved))

        @pl.when((bond > 0) & (d > 0))
        def _():
            shift_copy(d - 1).start()

        @pl.when((bond < last) & (d > 1))
        def _():
            pass_on(d - 2)

        @pl.when((bond < last) & (d > 2))
        def _():
            pass_near(d - 3)

        return carry

    pending[...] = jnp.zeros_like(pending)
    factor[...] = jnp.zeros_like(factor)
    coeff[...] = jnp.zeros_like(coeff)
    gram_copy(0).wait()
    diagonal[...] = (gram_own[:LANES, :LANES] + gram_in[:LANES, :LANES]) * scale + ones * ridge
    lax.fori_loop(0, blocks // 2, functools.partial(eliminate, rank // 2), 0)
    lax.fori_loop(blocks // 2, blocks, functools.partial(eliminate, rank), 0)
    finish(blocks - 1, rank)

    @pl.when(bond > 0)
    def _():
        shift_copy(blocks - 1).start()
        for j in range(1, slots):
            direct_copy(j).start()


    right_copy = pltpu.make_async_remote_copy(
        src_ref=right_out,
        dst_ref=right_in,
        send_sem=right_send,
        recv_sem=right_recv,
        device_id={"row": near},
        device_id_type=MESH,
    )

    right_scale = 1.0 / math.sqrt(2.0 * bond_dim)

    def project(who, store):
        ranks = pl.ds(pl.multiple_of(who * own_rank, own_rank), own_rank)

        def columns(cb, carry):
            at = pl.ds(pl.multiple_of(cb * TILE, TILE), TILE)
            store(at, dot(flat[ranks, :], theta[:, at]) * right_scale)
            return carry

        lax.fori_loop(0, 2 * bond_dim // TILE, columns, 0)

    def give(at, value):
        right_out[:, at] = value.astype(BF16)

    def keep(at, value):
        right_ref[:, at] = (value + right_in[:, at].astype(F32)).astype(BF16)

    pair_ranks = pl.ds(pl.multiple_of(slot * 2 * own_rank, 2 * own_rank), 2 * own_rank)
    for j in range(1, slots):
        at = pl.ds(pl.multiple_of(lax.rem(slot + j, slots) * block_rows, block_rows), block_rows)
        flat[pair_ranks, at] = (
            dot(high_all[pair_ranks, :], w_tall[:, at]) + dot(low_all[pair_ranks, :], w_tall[:, at])
        ).astype(BF16)

    project(near, give)
    right_copy.start()

    @pl.when(bond < last)
    def _():
        pass_on(blocks - 2)
        pass_near(blocks - 3)

    turn = interleave(block_rows)
    for d in range(0, blocks, 2):
        pair_of = [jnp.concatenate([left_ref[d + i, 0], left_ref[d + i, 1]], axis=0) for i in range(2)]
        left_out[:, d * LANES:(d + 2) * LANES] = dot(turn, jnp.concatenate(pair_of, axis=1)).astype(BF16)

    right_copy.wait()
    project(me, keep)

    @pl.when(bond < last)
    def _():
        pass_near(blocks - 2)
        shift_copy(blocks - 1).wait_recv()
        near_copy(0, blocks - 1, parity).start()

    @pl.when(bond < last)
    def _():
        stacked = jnp.concatenate([right_ref[:, :bond_dim], right_ref[:, bond_dim:]], axis=0)
        right_view[...] = dot(interleave(2 * own_rank), stacked).astype(BF16)
        odd_scale = 1.0 / math.sqrt(1.0 * bond_dim)

        def pair(d):
            for j in range(slots):
                near_copy(j, d, 1 - parity).wait_recv()
            both = jnp.concatenate([ahead[d, 0], ahead[d, 1]], axis=1)
            value = (dot(right_view[...], both) * odd_scale).astype(BF16)
            odd_ref[:, pl.ds(pl.multiple_of(d * LANES, LANES), LANES)] = value[:, :LANES]
            odd_ref[:, pl.ds(pl.multiple_of(rank + d * LANES, LANES), LANES)] = value[:, LANES:]

        def pairs(d, carry):
            pair(d)
            return carry

        lax.fori_loop(0, blocks - 1, pairs, 0)
        for j in range(1, slots):
            direct_arrival(j).wait_recv()
            near_copy(j, blocks - 1, parity).start()
        pair(blocks - 1)

        def sent(d, carry):
            for j in range(slots):
                near_copy(j, d, parity).wait_send()
            return carry

        def sent_far(d, carry):
            for j in range(1, slots):
                far_copy(j, d).wait_send()
            return carry

        lax.fori_loop(0, blocks - 1, sent_far, 0)

        lax.fori_loop(0, blocks, sent, 0)

    @pl.when(bond == last)
    def _():
        odd_ref[...] = jnp.zeros_like(odd_ref)

    @pl.when(bond > 0)
    def _():
        def sent(d, carry):
            shift_copy(d).wait_send()
            return carry

        lax.fori_loop(0, blocks, sent, 0)
        for j in range(1, slots):
            direct_copy(j).wait_send()

    for mask in [0] + omega_order:
        for bit in lower_bits(mask):
            omega_copy(mask, bit).wait_send()
    for mask in [0] + b_order:
        for s in b_lower(mask):
            for k in range(CHUNKS):
                b_copy(mask, s, k).wait_send()
    for j in range(1, slots):
        for q in range(PARTS):
            a_copy(j, q).wait_send()


def layer(gate, left_site, right_site, omega, n, bonds):
    block_rows, bond_dim = left_site.shape
    part_rows = block_rows // PARTS
    depth = right_site.shape[0]
    drawn, rank = omega.shape
    slots = n // 2
    rows = slots * block_rows
    half = block_rows // 2
    own_rank = rank // n
    blocks = rank // LANES
    dma = pltpu.SemaphoreType.DMA
    return pl.pallas_call(
        functools.partial(layer_kernel, n, bonds),
        out_shape=(
            jax.ShapeDtypeStruct((block_rows, rank), BF16),
            jax.ShapeDtypeStruct((own_rank, 2 * bond_dim), BF16),
            jax.ShapeDtypeStruct((2 * own_rank, 2 * rank), BF16),
        ),
        in_specs=[pl.BlockSpec(memory_space=pltpu.HBM)] * 4,
        out_specs=(pl.BlockSpec(memory_space=pltpu.VMEM),) * 3,
        scratch_shapes=[
            pltpu.VMEM((slots, PARTS, part_rows, bond_dim), BF16),
            pltpu.VMEM((part_rows, bond_dim), BF16),
            pltpu.VMEM((n * depth, 2 * bond_dim), BF16),
            pltpu.VMEM((bonds * n * drawn, rank), omega.dtype),
            pltpu.VMEM((rows, 2 * bond_dim), BF16),
            pltpu.VMEM((rows, rank), BF16),
            pltpu.VMEM((rank, rows), BF16),
            pltpu.VMEM((rank, rank), BF16),
            pltpu.VMEM((rank, rank), BF16),
            pltpu.VMEM((rank, rank), F32),
            pltpu.VMEM((rank, rank), F32),
            pltpu.VMEM((LANES, LANES), F32),
            pltpu.VMEM((LANES, rank), F32),
            pltpu.VMEM((LANES, 3 * LANES), BF16),
            pltpu.VMEM((2 * LANES, rank), BF16),
            pltpu.VMEM((rank, rows), BF16),
            pltpu.VMEM((blocks, 2, half, LANES), BF16),
            pltpu.VMEM((blocks, 2, n * half, LANES), BF16),
            pltpu.VMEM((own_rank, 2 * bond_dim), BF16),
            pltpu.VMEM((own_rank, 2 * bond_dim), BF16),
            pltpu.VMEM((2 * own_rank, bond_dim), BF16),
            pltpu.VMEM((SUB, LANES), F32),
            pltpu.VMEM((SUB, LANES), F32),
            dma((bonds * n,)), dma((bonds * n,)),
            dma((n, CHUNKS)), dma((n, CHUNKS)),
            dma((slots, PARTS)), dma((slots, PARTS)),
            dma((blocks,)), dma((blocks,)),
            dma, dma,
            dma((blocks,)), dma((blocks,)),
            dma((slots, blocks)), dma((slots, blocks)),
            dma((slots, blocks)), dma((slots, blocks)),
            dma, dma,
            dma((slots,)), dma((slots,)),
            dma((2 + PARTS,)), dma,
            pltpu.SMEM(gate.shape, F32),
        ],
        compiler_params=pltpu.CompilerParams(
            collective_id=0, has_side_effects=True, vmem_limit_bytes=62 * 1024 * 1024
        ),
        name="layer",
    )(gate, left_site, right_site, omega)


def shards(left_site, right_site, gate, omega):
    n, bonds = lax.axis_size("row"), lax.axis_size("bond")
    if omega.shape[0] % 16:
        omega = omega.astype(F32)
    return layer(gate, left_site, right_site, omega, n, bonds)


def solution(mesh):
    split_rows = P(("bond", "row"), None)
    return jax.shard_map(
        shards,
        mesh=mesh,
        in_specs=(split_rows, split_rows, P(), split_rows),
        out_specs=(split_rows, split_rows, split_rows),
        check_vma=False,
    )
```
